32 devices in a mesh: group: 2 (over y), station: 4 (over z), tm: 2 (over x), chan: 2 (over core).
Axes of the slice: x: 2, y: 2, z: 4, core: 2. Of those that a mesh axis runs over, the one named last changes fastest.
Arguments:
- voltages: bfloat16 [8, 128, 2, 96, 256], P(('group', 'station'), 'chan', None, None, 'tm'), parts along dimension 0, may hold values from -6 to 6
- delays: int32 [8], P(('group', 'station')), parts along dimension 0, may hold values from 0 to 16, as said below
- tap_sets: int32 [8, 128], P(('group', 'station'), 'chan'), parts along dimension 0, may hold values from 0 to 15
- tap_table: bfloat16 [16, 16], replicated, may hold values from -1.5 to 1.5
- weights: bfloat16 [8, 128, 2, 96, 128], P(('group', 'station'), 'chan'), parts along dimension 0, may hold values from -0.3125 to 0.3125
Outputs:
- array_beams: bfloat16 [256, 2, 128, 256], P(('group', 'chan', 'station'), None, None, 'tm'), parts along dimension 0
The draws below stay inside these ranges and needn't reach their ends.
There are 2 independent parts, one for each index of `group`. The reference program is written for one: setup_inputs(seed, part) draws one part's arguments, and reference() takes and returns one part's arrays. A program takes and returns all parts, laid end to end along the dimension named above; an argument that names none is the same for every part. Nothing has to cross between parts.
Inputs may be any that keep to these rules, and one draw needn't show every extreme that they name: `delays`: every delay lies in 0 to 16, and some station has delay 16.
All inputs are finite; a program needn't handle non-finite values.
Results may differ from the reference program's by a relative error of at most 0.0049.
Values may be sent and summed in bfloat16 or wider, within the bound.
A program may use at most 64 MiB of HBM per device.

```python
import jax
import jax.numpy as jnp
from jax import lax

ANTENNA_COUNT = 96
BEAM_TOTAL = 128
TAPS = 16
MAXD = 16
NSETS = 16
STATION_TOTAL = 4
FREQUENCY_BINS = 128
TIME_SAMPLES = 256


def draw_delays(key, part):
    drawn = jax.random.randint(key, (STATION_TOTAL,), 0, MAXD + 1)
    chosen = jax.random.randint(jax.random.fold_in(key, 7), (), 0, STATION_TOTAL)
    positions = jnp.arange(STATION_TOTAL)
    return jnp.where(positions == chosen, MAXD, drawn).astype(jnp.int32)


def plant(array, own_key, least, largest):
    longest = array.shape.index(max(array.shape))
    spots = []
    for shift in (0, 1):
        where = [jax.random.randint(jax.random.fold_in(own_key, axis), (), 0, length) for axis, length in enumerate(array.shape)]
        where[longest] = (where[longest] + shift) % array.shape[longest]
        spots.append(tuple(where))
    return array.at[spots[0]].set(least).at[spots[1]].set(largest)


def raised(values, key, source, target, shards_of, factor):
    def block_of(axis_at):
        return (jnp.arange(values.shape[axis_at]) // (values.shape[axis_at] // shards_of)).reshape((-1,) + (1,) * (values.ndim - 1 - axis_at))

    near = jax.random.permutation(key, shards_of)[block_of(target)]
    other_side = (block_of(target) + shards_of // 2) % shards_of
    return jnp.where((block_of(source) == near) | (block_of(source) == other_side), factor * values, values)


def levels(key, dims, cuts, low, top_value):
    def one(dim, parts):
        heights = jax.random.uniform(jax.random.fold_in(jax.random.fold_in(key, 6), dim), (parts,), jnp.float32, low / len(cuts), top_value / len(cuts))
        return jnp.repeat(jnp.exp(heights), dims[dim] // parts).reshape((-1,) + (1,) * (len(dims) - dim - 1))

    level = one(*cuts[0])
    for cut in cuts[1:]:
        level = level * one(*cut)
    return level


def gaussian(own_key, dims, width, reach, pieces=(), dtype=jnp.bfloat16):
    loudness = levels(own_key, dims, pieces, -0.22, 0.18) if pieces else 1.0
    array = jax.random.normal(own_key, dims, jnp.float32) * width * loudness
    return jnp.minimum(jnp.maximum(array, -reach), reach).astype(dtype)


def bell_draw_with(key, shape, spread, reach, split, heavy, held_as=jnp.bfloat16):
    values = spread * jax.random.normal(key, shape, jnp.float32)
    if split:
        values = values * levels(key, shape, split, -0.22, 0.18)
    return jnp.clip(raised(values, jax.random.fold_in(key, 3), *heavy), -reach, reach).astype(held_as)


def setup_inputs(seed: int = 0, part: int = 0) -> dict:
    key_of = jax.random.split(jax.random.key(seed), 6)
    part_splits = jax.random.split(jax.random.fold_in(key_of[5], part), 6)
    voltages = gaussian(part_splits[0], (STATION_TOTAL, FREQUENCY_BINS, 2, ANTENNA_COUNT, TIME_SAMPLES), 1.0, 6.0, ((0, 4), (1, 2), (4, 2)))
    delays = draw_delays(jax.random.fold_in(jax.random.fold_in(key_of[5], part), 71), part)
    tap_sets = plant(jax.random.randint(part_splits[2], (STATION_TOTAL, FREQUENCY_BINS), 0, NSETS), jax.random.fold_in(part_splits[2], 1), 0, NSETS - 1).astype(jnp.int32)
    tap_table = gaussian(key_of[3], (NSETS, TAPS), 0.25, 1.5)
    weights = bell_draw_with(part_splits[4], (STATION_TOTAL, FREQUENCY_BINS, 2, ANTENNA_COUNT, BEAM_TOTAL), (2 * ANTENNA_COUNT * STATION_TOTAL) ** -0.5, 0.3125, ((0, 4), (1, 2)), (0, 1, 4, 2.0))
    return {"voltages": voltages, "delays": delays, "tap_sets": tap_sets, "tap_table": tap_table, "weights": weights}


def reference(voltages, delays, tap_sets, tap_table, weights):
    halo_len = MAXD + TAPS - 1
    table_f32 = tap_table.astype(jnp.float32)

    def one_station(running, station_item):
        samples, delay_now, chosen_sets, steer = station_item
        samples_f32 = samples.astype(jnp.float32)
        padded = jnp.pad(samples_f32, ((0, 0), (0, 0), (0, 0), (halo_len, 0)))
        coefficients = table_f32[chosen_sets]
        summed_taps = jnp.zeros(samples_f32.shape, jnp.float32)
        for tap_index in range(TAPS):
            begin = (halo_len - delay_now - tap_index).astype(jnp.int32)
            shifted = lax.dynamic_slice_in_dim(padded, begin, TIME_SAMPLES, 3)
            summed_taps = summed_taps + coefficients[:, tap_index][:, None, None, None] * shifted
        delayed_voltages = lax.optimization_barrier(summed_taps.astype(jnp.bfloat16)).astype(jnp.float32)
        steer_f32 = steer.astype(jnp.float32)
        real_in = delayed_voltages[:, 0]
        imag_in = delayed_voltages[:, 1]
        real_part = jnp.einsum('cat,cab->cbt', real_in, steer_f32[:, 0]) - jnp.einsum('cat,cab->cbt', imag_in, steer_f32[:, 1])
        imag_part = jnp.einsum('cat,cab->cbt', real_in, steer_f32[:, 1]) + jnp.einsum('cat,cab->cbt', imag_in, steer_f32[:, 0])
        return running + jnp.stack([real_part, imag_part], axis=1), None

    start_sum = jnp.zeros((FREQUENCY_BINS, 2, BEAM_TOTAL, TIME_SAMPLES), jnp.float32)
    result, unused = lax.scan(one_station, start_sum, (voltages, delays, tap_sets, weights))
    return result.astype(jnp.bfloat16)
```

```python
import functools

import jax
import jax.numpy as jnp
from jax import lax
from jax.experimental import pallas as pl
from jax.experimental.pallas import tpu as pltpu
from jax.sharding import PartitionSpec as P

MAXD = 16
MESH = pl.DeviceIdType.MESH
LEAD = 4
LAG = 4


def kernel(
    n, tm_count, sizes, sets_hbm, delays_hbm, taps_hbm, v_hbm, w_hbm, out_buf,
    sets, delays, taps, spread, lags, v_buf, w_buf, band, halo_out, halo_in,
    acc_out, acc_in, own,
    small_sem, v_sem, w_sem, hs_sem, hr_sem, as_sem, ar_sem,
):
    channels, parts, antennas, beams, time_len, pad = sizes
    rows = channels // n
    rows_in = parts * antennas
    folds = time_len // pad
    fold_rows = rows_in // folds
    set_count, tap_count = taps.shape
    bf16, f32 = jnp.bfloat16, jnp.float32

    me = lax.axis_index("station")
    tm = lax.axis_index("tm")
    later, earlier = lax.rem(tm + 1, tm_count), lax.rem(tm + tm_count - 1, tm_count)

    flip = jnp.where(me >= n // 2, 1, 0)
    place = me + flip * (n - 1 - 2 * me)
    ahead_dir, back_dir = flip, 1 - flip
    ahead_count = (n - 1 - place) * rows
    back_count = (place + 1) * rows
    offset = LAG + ahead_count - back_count

    def channel_of(station, k):
        return (station + flip * (n - 1 - 2 * station)) * rows + k

    def ahead_channel(i):
        return channel_of(n - 1 - i // rows, lax.rem(i, rows))

    def back_channel(j):
        return channel_of(j // rows, lax.rem(j, rows))

    def v_copy(ch):
        return pltpu.make_async_copy(v_hbm.at[ch], v_buf.at[ch], v_sem.at[ch])

    def w_copy(ch):
        return pltpu.make_async_copy(w_hbm.at[ch], w_buf.at[ch], w_sem.at[ch])

    def halo_copy(ch):
        return pltpu.make_async_remote_copy(
            src_ref=halo_out.at[ch],
            dst_ref=halo_in.at[ch],
            send_sem=hs_sem.at[ch],
            recv_sem=hr_sem.at[ch],
            device_id={"tm": later},
            device_id_type=MESH,
        )

    def sum_copy(ch, direction):
        target = me + 1 - 2 * direction
        final = (ch // rows == target) & (direction == 1)
        slot = jnp.where(final, channels + lax.rem(ch, rows), ch)
        return pltpu.make_async_remote_copy(
            src_ref=acc_out.at[ch],
            dst_ref=acc_in.at[slot],
            send_sem=as_sem.at[ch],
            recv_sem=ar_sem.at[slot],
            device_id={"station": target},
            device_id_type=MESH,
        )

    def arrival(ch, direction):
        final = (ch // rows == me) & (direction == 1)
        return jnp.where(final, channels + lax.rem(ch, rows), ch)

    def wait_arrival(slot):
        pltpu.make_async_copy(acc_in.at[slot], acc_in.at[slot], ar_sem.at[slot]).wait()

    barrier = pltpu.get_barrier_semaphore()
    for target in ({"tm": earlier}, {"tm": later}):
        pl.semaphore_signal(barrier, inc=1, device_id=target, device_id_type=MESH)

    @pl.when(me > 0)
    def _():
        pl.semaphore_signal(barrier, inc=1, device_id={"station": me - 1}, device_id_type=MESH)

    @pl.when(me < n - 1)
    def _():
        pl.semaphore_signal(barrier, inc=1, device_id={"station": me + 1}, device_id_type=MESH)

    small = [
        pltpu.make_async_copy(sets_hbm, sets, small_sem.at[0]),
        pltpu.make_async_copy(delays_hbm, delays, small_sem.at[1]),
        pltpu.make_async_copy(taps_hbm, taps, small_sem.at[2]),
    ]
    for copy in small:
        copy.start()

    def load(ch):
        v_copy(ch).start()
        w_copy(ch).start()

    for i in range(LEAD):
        load(ahead_channel(i))

    from_row = lax.broadcasted_iota(jnp.int32, (folds * time_len, time_len), 0)
    to_lane = lax.broadcasted_iota(jnp.int32, (folds * time_len, time_len), 1)
    wanted = (to_lane // pad) * time_len + lax.rem(to_lane, pad) + time_len - pad
    picker = (from_row == wanted).astype(f32).astype(bf16)

    def pack(ch):
        v_copy(ch).wait()
        wide = jnp.concatenate(
            [v_buf[ch, pl.ds(q * fold_rows, fold_rows), :] for q in range(folds)], axis=1
        )
        halo_out[ch] = jnp.dot(wide, picker, preferred_element_type=f32).astype(bf16)
        halo_copy(ch).start()

    present = 2 + jnp.where(me > 0, 1, 0) + jnp.where(me < n - 1, 1, 0)
    pl.semaphore_wait(barrier, present)

    for i in range(LEAD):
        pack(ahead_channel(i))

    for copy in small:
        copy.wait()

    pick_tap = lax.broadcasted_iota(jnp.int32, (tap_count, tap_count * 128), 1) // 128
    tap_row = lax.broadcasted_iota(jnp.int32, (tap_count, tap_count * 128), 0)
    chosen = (pick_tap == tap_row).astype(f32).astype(bf16)
    values = jnp.dot(taps[...], chosen, preferred_element_type=f32)
    for m in range(set_count):
        spread[m] = values[m:m + 1]

    out_pos = lax.broadcasted_iota(jnp.int32, (time_len, 2 * time_len), 0)
    column = lax.broadcasted_iota(jnp.int32, (time_len, 2 * time_len), 1)
    in_pos = jnp.where(column < time_len, column, lax.rem(column, pad) - pad)
    usable = (column < time_len) | (tm > 0)
    lags[...] = jnp.where(usable, out_pos - delays[0] - in_pos, -1)

    def make_band(m, carry):
        lag = lags[...]
        values = jnp.zeros((time_len, 2 * time_len), f32)
        for k in range(tap_count):
            tap = spread[m, :, pl.ds(k * 128, 128)]
            tap = jnp.concatenate([tap] * (2 * time_len // 128), axis=1)
            values = jnp.where(lag == k, tap, values)
        band[m] = values.astype(bf16)
        return carry

    lax.fori_loop(0, set_count, make_band, 0)

    def load_rest(i, carry):
        @pl.when(i < ahead_count)
        def _():
            load(ahead_channel(i))

        j = i - LEAD
        @pl.when(j < back_count)
        def _():
            load(back_channel(j))

        return carry

    lax.fori_loop(LEAD, jnp.maximum(ahead_count, back_count + LEAD), load_rest, 0)

    fold_lane = lax.broadcasted_iota(jnp.int32, (fold_rows, time_len), 1) // pad

    def beams_of(ch):
        halo_copy(ch).wait_recv()
        w_copy(ch).wait()
        rim = halo_in[ch]
        rims = jnp.concatenate(
            [jnp.where(fold_lane == q, rim, jnp.zeros_like(rim)) for q in range(folds)], axis=0
        )
        window = jnp.concatenate([v_buf[ch], rims], axis=1)
        delayed = lax.dot_general(
            band[sets[0, ch]], window, (((1,), (1,)), ((), ())), preferred_element_type=f32
        ).astype(bf16)
        wr = w_buf[ch, pl.ds(0, antennas), :]
        wi = w_buf[ch, pl.ds(antennas, antennas), :]
        steer = jnp.concatenate(
            [jnp.concatenate([wr, wi], axis=1), jnp.concatenate([-wi, wr], axis=1)], axis=0
        )
        return jnp.dot(delayed, steer, preferred_element_type=f32)

    def step(i, carry):
        j = i - offset

        @pl.when(i + LEAD < ahead_count)
        def _():
            pack(ahead_channel(i + LEAD))

        @pl.when((j + LEAD >= 0) & (j + LEAD < back_count))
        def _():
            pack(back_channel(j + LEAD))

        @pl.when(i < ahead_count)
        def _():
            ch = ahead_channel(i)
            total = beams_of(ch)

            @pl.when(place > 0)
            def _():
                wait_arrival(ch)
                acc_out[ch] = (total + acc_in[ch].astype(f32)).astype(bf16)

            @pl.when(place == 0)
            def _():
                acc_out[ch] = total.astype(bf16)

            sum_copy(ch, ahead_dir).start()

        @pl.when((j >= 0) & (j < back_count))
        def _():
            ch = back_channel(j)
            total = beams_of(ch)
            slot = arrival(ch, back_dir)
            wait_arrival(slot)
            total = total + acc_in[slot].astype(f32)

            @pl.when(j < place * rows)
            def _():
                acc_out[ch] = total.astype(bf16)
                sum_copy(ch, back_dir).start()

            @pl.when(j >= place * rows)
            def _():
                own[lax.rem(j, rows)] = total

        return carry

    lax.fori_loop(0, ahead_count + LAG, step, 0)

    def finish(k, carry):
        slot = arrival(me * rows + k, ahead_dir)

        @pl.when(place > 0)
        def _():
            wait_arrival(slot)
            out_buf[k] = (own[k] + acc_in[slot].astype(f32)).T.astype(bf16)

        @pl.when(place == 0)
        def _():
            out_buf[k] = own[k].T.astype(bf16)

        return carry

    lax.fori_loop(0, rows, finish, 0)

    def drain_halo(ch, carry):
        halo_copy(ch).wait_send()
        return carry

    lax.fori_loop(0, channels, drain_halo, 0)

    def drain_ahead(i, carry):
        sum_copy(ahead_channel(i), ahead_dir).wait_send()
        return carry

    lax.fori_loop(0, ahead_count, drain_ahead, 0)

    def drain_back(j, carry):
        sum_copy(back_channel(j), back_dir).wait_send()
        return carry

    lax.fori_loop(0, place * rows, drain_back, 0)


def body(voltages, delays, tap_sets, tap_table, weights):
    _, channels, parts, antennas, time_len = voltages.shape
    beams = weights.shape[-1]
    set_count, tap_count = tap_table.shape
    n = lax.axis_size("station")
    tm_count = lax.axis_size("tm")
    rows = channels // n
    pad = MAXD + tap_count
    rows_in = parts * antennas
    fold_rows = rows_in * pad // time_len
    sizes = (channels, parts, antennas, beams, time_len, pad)
    bf16, f32 = jnp.bfloat16, jnp.float32
    dma = pltpu.SemaphoreType.DMA
    in_hbm = pl.BlockSpec(memory_space=pltpu.HBM)
    result = pl.pallas_call(
        functools.partial(kernel, n, tm_count, sizes),
        out_shape=jax.ShapeDtypeStruct((rows, 2 * beams, time_len), bf16),
        in_specs=[in_hbm] * 5,
        out_specs=pl.BlockSpec(memory_space=pltpu.VMEM),
        scratch_shapes=[
            pltpu.SMEM(tap_sets.shape, jnp.int32),
            pltpu.SMEM(delays.shape, jnp.int32),
            pltpu.VMEM((set_count, tap_count), bf16),
            pltpu.VMEM((set_count, 1, tap_count * 128), f32),
            pltpu.VMEM((time_len, 2 * time_len), jnp.int32),
            pltpu.VMEM((channels, rows_in, time_len), bf16),
            pltpu.VMEM((channels, rows_in, beams), bf16),
            pltpu.VMEM((set_count, time_len, 2 * time_len), bf16),
            pltpu.VMEM((channels, fold_rows, time_len), bf16),
            pltpu.VMEM((channels, fold_rows, time_len), bf16),
            pltpu.VMEM((channels, time_len, 2 * beams), bf16),
            pltpu.VMEM((channels + rows, time_len, 2 * beams), bf16),
            pltpu.VMEM((rows, time_len, 2 * beams), f32),
            dma((3,)),
            dma((channels,)),
            dma((channels,)),
            dma((channels,)),
            dma((channels,)),
            dma((channels,)),
            dma((channels + rows,)),
        ],
        compiler_params=pltpu.CompilerParams(
            collective_id=0, has_side_effects=True, vmem_limit_bytes=60 * 1024 * 1024
        ),
    )(
        tap_sets,
        delays,
        tap_table,
        voltages.reshape(channels, rows_in, time_len),
        weights.reshape(channels, rows_in, beams),
    )
    return result.reshape(rows, 2, beams, time_len)


def solution(mesh):
    return jax.shard_map(
        body,
        mesh=mesh,
        in_specs=(
            P(("group", "station"), "chan", None, None, "tm"),
            P(("group", "station")),
            P(("group", "station"), "chan"),
            P(),
            P(("group", "station"), "chan", None, None, None),
        ),
        out_specs=P(("group", "chan", "station"), None, None, "tm"),
        check_vma=False,
    )
```

```python
import functools

import jax
import jax.numpy as jnp
from jax import lax
from jax.experimental import pallas as pl
from jax.experimental.pallas import tpu as pltpu
from jax.sharding import PartitionSpec as P

MAXD = 16
MESH = pl.DeviceIdType.MESH
LEAD = 4
LAG = 4


def kernel(
    n, tm_count, sizes, sets_hbm, delays_hbm, taps_hbm, v_hbm, w_hbm, out_buf,
    sets, delays, taps, spread, own_lag, rim_lag, v_buf, w_buf, halo_out, halo_in,
    acc_out, acc_in, own,
    small_sem, v_sem, w_sem, hs_sem, hr_sem, as_sem, ar_sem, bs_sem, br_sem,
):
    channels, parts, antennas, beams, time_len, pad, group = sizes
    rows = channels // n
    rows_in = parts * antennas
    folds = time_len // pad
    fold_rows = rows_in // folds
    set_count, tap_count = taps.shape
    head = group if n > 2 else 0
    bf16, f32 = jnp.bfloat16, jnp.float32

    me = lax.axis_index("station")
    tm = lax.axis_index("tm")
    later, earlier = lax.rem(tm + 1, tm_count), lax.rem(tm + tm_count - 1, tm_count)

    flip = jnp.where(me >= n // 2, 1, 0)
    place = me + flip * (n - 1 - 2 * me)
    ahead_dir, back_dir = flip, 1 - flip
    ahead_count = (n - 1 - place) * rows
    back_count = (place + 1) * rows
    offset = LAG + ahead_count - back_count
    start = jnp.where(place == 0, head, 0)

    def channel_of(station, k):
        return (station + flip * (n - 1 - 2 * station)) * rows + k

    def ahead_channel(i):
        return channel_of(n - 1 - i // rows, lax.rem(i, rows))

    def back_channel(j):
        return channel_of(j // rows, lax.rem(j, rows))

    def v_copy(g):
        span = pl.ds(g * group, group)
        return pltpu.make_async_copy(v_hbm.at[span], v_buf.at[span], v_sem.at[g])

    def w_copy(g):
        span = pl.ds(g * group, group)
        return pltpu.make_async_copy(w_hbm.at[span], w_buf.at[span], w_sem.at[g])

    def halo_copy(ch):
        return pltpu.make_async_remote_copy(
            src_ref=halo_out.at[ch],
            dst_ref=halo_in.at[ch],
            send_sem=hs_sem.at[ch],
            recv_sem=hr_sem.at[ch],
            device_id={"tm": later},
            device_id_type=MESH,
        )

    def sum_copy(ch, direction):
        target = me + 1 - 2 * direction
        final = (ch // rows == target) & (direction == 1)
        slot = jnp.where(final, channels + lax.rem(ch, rows), ch)
        return pltpu.make_async_remote_copy(
            src_ref=acc_out.at[ch],
            dst_ref=acc_in.at[slot],
            send_sem=as_sem.at[ch],
            recv_sem=ar_sem.at[slot],
            device_id={"station": target},
            device_id_type=MESH,
        )

    def arrival(ch, direction):
        final = (ch // rows == me) & (direction == 1)
        return jnp.where(final, channels + lax.rem(ch, rows), ch)

    def wait_arrival(slot):
        pltpu.make_async_copy(acc_in.at[slot], acc_in.at[slot], ar_sem.at[slot]).wait()

    late_rows, early_rows = pl.ds(pad, time_len - pad), pl.ds(0, pad)

    def late_copy(i):
        ch = ahead_channel(i)
        return pltpu.make_async_remote_copy(
            src_ref=acc_out.at[ch, late_rows],
            dst_ref=acc_in.at[ch, late_rows],
            send_sem=as_sem.at[ch],
            recv_sem=ar_sem.at[ch],
            device_id={"station": me + 1 - 2 * ahead_dir},
            device_id_type=MESH,
        )

    def early_copy(i):
        ch = ahead_channel(i)
        return pltpu.make_async_remote_copy(
            src_ref=acc_out.at[ch, early_rows],
            dst_ref=acc_in.at[ch, early_rows],
            send_sem=bs_sem.at[i],
            recv_sem=br_sem.at[i],
            device_id={"station": me + 1 - 2 * ahead_dir},
            device_id_type=MESH,
        )

    small = [
        pltpu.make_async_copy(taps_hbm, taps, small_sem.at[0]),
        pltpu.make_async_copy(delays_hbm, delays, small_sem.at[1]),
        pltpu.make_async_copy(sets_hbm, sets, small_sem.at[2]),
    ]
    for copy in small:
        copy.start()
    first_group = ahead_channel(0) // group
    v_copy(first_group).start()
    w_copy(first_group).start()

    barrier = pltpu.get_barrier_semaphore()

    @pl.when(me > 0)
    def _():
        pl.semaphore_signal(barrier, inc=1, device_id={"station": me - 1}, device_id_type=MESH)

    @pl.when(me < n - 1)
    def _():
        pl.semaphore_signal(barrier, inc=1, device_id={"station": me + 1}, device_id_type=MESH)

    for target in ({"tm": earlier}, {"tm": later}):
        pl.semaphore_signal(barrier, inc=1, device_id=target, device_id_type=MESH)

    def load_ahead(g, carry):
        v_copy(ahead_channel(g * group) // group).start()
        w_copy(ahead_channel(g * group) // group).start()
        return carry

    def load_back(g, carry):
        v_copy(back_channel(g * group) // group).start()
        w_copy(back_channel(g * group) // group).start()
        return carry

    lax.fori_loop(1, ahead_count // group, load_ahead, 0)
    lax.fori_loop(0, back_count // group, load_back, 0)

    from_row = lax.broadcasted_iota(jnp.int32, (folds * time_len, time_len), 0)
    to_lane = lax.broadcasted_iota(jnp.int32, (folds * time_len, time_len), 1)
    wanted = (to_lane // pad) * time_len + lax.rem(to_lane, pad) + time_len - pad
    picker = (from_row == wanted).astype(f32).astype(bf16)

    for copy in small:
        copy.wait()

    pick_tap = lax.broadcasted_iota(jnp.int32, (tap_count, tap_count * 128), 1) // 128
    tap_row = lax.broadcasted_iota(jnp.int32, (tap_count, tap_count * 128), 0)
    chosen = (pick_tap == tap_row).astype(f32).astype(bf16)
    values = jnp.dot(taps[...], chosen, preferred_element_type=f32)
    for m in range(set_count):
        spread[m] = values[m:m + 1]

    out_pos = lax.broadcasted_iota(jnp.int32, (time_len, time_len), 0)
    in_pos = lax.broadcasted_iota(jnp.int32, (time_len, time_len), 1)
    own_lag[...] = out_pos - in_pos - delays[0]
    rim_out = lax.broadcasted_iota(jnp.int32, (pad, time_len), 0)
    rim_in = lax.rem(lax.broadcasted_iota(jnp.int32, (pad, time_len), 1), pad) - pad
    rim_lag[...] = jnp.where(tm > 0, rim_out - rim_in - delays[0], -1)

    fold_lane = lax.broadcasted_iota(jnp.int32, (fold_rows, time_len), 1) // pad

    def toeplitz(m, lag):
        values = jnp.zeros(lag.shape, f32)
        for k in range(tap_count):
            values = jnp.where(lag == k, spread[m, :, pl.ds(k * 128, 128)], values)
        return values.astype(bf16)

    def rims_of(ch):
        rim = halo_in[ch]
        return jnp.concatenate(
            [jnp.where(fold_lane == q, rim, jnp.zeros_like(rim)) for q in range(folds)], axis=0
        )

    def filtered(filt, window):
        return lax.dot_general(
            filt, window, (((1,), (1,)), ((), ())), preferred_element_type=f32
        ).astype(bf16)

    def steered(ch, delayed):
        wr = w_buf[ch, pl.ds(0, antennas), :]
        wi = w_buf[ch, pl.ds(antennas, antennas), :]
        steer = jnp.concatenate(
            [jnp.concatenate([wr, wi], axis=1), jnp.concatenate([-wi, wr], axis=1)], axis=0
        )
        return jnp.dot(delayed, steer, preferred_element_type=f32)

    def beams_of(ch):
        halo_copy(ch).wait_recv()
        m = sets[0, ch]
        rim = toeplitz(m, rim_lag[...])
        rim = jnp.concatenate([rim, jnp.zeros((time_len - pad, time_len), bf16)], axis=0)
        filt = jnp.concatenate([toeplitz(m, own_lag[...]), rim], axis=1)
        window = jnp.concatenate([v_buf[ch], rims_of(ch)], axis=1)
        return steered(ch, filtered(filt, window))

    def pack(ch):
        wide = jnp.concatenate(
            [v_buf[ch, pl.ds(q * fold_rows, fold_rows), :] for q in range(folds)], axis=1
        )
        halo_out[ch] = jnp.dot(wide, picker, preferred_element_type=f32).astype(bf16)
        halo_copy(ch).start()

    def pack_ahead(i):
        ch = ahead_channel(i)

        @pl.when(lax.rem(i, group) == 0)
        def _():
            v_copy(ch // group).wait()

        pack(ch)

    def pack_back(j):
        ch = back_channel(j)

        @pl.when(lax.rem(j, group) == 0)
        def _():
            v_copy(ch // group).wait()

        pack(ch)

    present = 2 + jnp.where(me > 0, 1, 0) + jnp.where(me < n - 1, 1, 0)
    pl.semaphore_wait(barrier, present)

    if head:
        @pl.when(place == 0)
        def _():
            v_copy(first_group).wait()
            w_copy(first_group).wait()

            def send_late(i, carry):
                ch = ahead_channel(i)
                filt = toeplitz(sets[0, ch], own_lag[late_rows, :])
                total = steered(ch, filtered(filt, v_buf[ch]))
                acc_out[ch, late_rows, :] = total.astype(bf16)
                late_copy(i).start()
                return carry

            lax.fori_loop(0, head, send_late, 0)

            def pack_head(i, carry):
                pack(ahead_channel(i))
                return carry

            lax.fori_loop(0, head, pack_head, 0)

    def pack_first(i, carry):
        pack_ahead(i)
        return carry

    lax.fori_loop(start, start + LEAD, pack_first, 0)

    if head:
        @pl.when(place == 0)
        def _():
            def send_early(i, carry):
                ch = ahead_channel(i)
                halo_copy(ch).wait_recv()
                m = sets[0, ch]
                filt = jnp.concatenate(
                    [toeplitz(m, own_lag[early_rows, :]), toeplitz(m, rim_lag[...])], axis=1
                )
                window = jnp.concatenate([v_buf[ch], rims_of(ch)], axis=1)
                total = steered(ch, filtered(filt, window))
                acc_out[ch, early_rows, :] = total.astype(bf16)
                early_copy(i).start()
                return carry

            lax.fori_loop(0, head, send_early, 0)

    def step(i, carry):
        j = i - offset

        @pl.when(i + LEAD < ahead_count)
        def _():
            pack_ahead(i + LEAD)

        @pl.when((j + LEAD >= 0) & (j + LEAD < back_count))
        def _():
            pack_back(j + LEAD)

        @pl.when(i < ahead_count)
        def _():
            ch = ahead_channel(i)

            @pl.when(lax.rem(i, group) == 0)
            def _():
                w_copy(ch // group).wait()

            total = beams_of(ch)

            @pl.when(place > 0)
            def _():
                cut = (place == 1) & (i < head)

                if head:
                    @pl.when(cut)
                    def _():
                        late_copy(i).wait_recv()
                        early_copy(jnp.where(cut, i, 0)).wait_recv()

                @pl.when(jnp.logical_not(cut))
                def _():
                    wait_arrival(ch)

                acc_out[ch] = (total + acc_in[ch].astype(f32)).astype(bf16)

            @pl.when(place == 0)
            def _():
                acc_out[ch] = total.astype(bf16)

            sum_copy(ch, ahead_dir).start()

        @pl.when((j >= 0) & (j < back_count))
        def _():
            ch = back_channel(j)

            @pl.when(lax.rem(j, group) == 0)
            def _():
                w_copy(ch // group).wait()

            total = beams_of(ch)
            slot = arrival(ch, back_dir)
            wait_arrival(slot)
            total = total + acc_in[slot].astype(f32)

            @pl.when(j < place * rows)
            def _():
                acc_out[ch] = total.astype(bf16)
                sum_copy(ch, back_dir).start()

            @pl.when(j >= place * rows)
            def _():
                own[lax.rem(j, rows)] = total

        return carry

    lax.fori_loop(start, ahead_count + LAG, step, 0)

    def drain_halo(ch, carry):
        halo_copy(ch).wait_send()
        return carry

    lax.fori_loop(0, channels, drain_halo, 0)

    def drain_back(j, carry):
        sum_copy(back_channel(j), back_dir).wait_send()
        return carry

    lax.fori_loop(0, place * rows, drain_back, 0)

    def drain_ahead(i, carry):
        sum_copy(ahead_channel(i), ahead_dir).wait_send()
        return carry

    @pl.when(place > 0)
    def _():
        lax.fori_loop(0, ahead_count, drain_ahead, 0)

        def finish(k, carry):
            slot = arrival(me * rows + k, ahead_dir)
            wait_arrival(slot)
            out_buf[k] = (own[k] + acc_in[slot].astype(f32)).T.astype(bf16)
            return carry

        lax.fori_loop(0, rows, finish, 0)

    @pl.when(place == 0)
    def _():
        def finish(k, carry):
            out_buf[k] = own[k].T.astype(bf16)
            return carry

        lax.fori_loop(0, rows, finish, 0)

        if head:
            def drain_head(i, carry):
                late_copy(i).wait_send()
                early_copy(i).wait_send()
                return carry

            lax.fori_loop(0, head, drain_head, 0)

        lax.fori_loop(head, ahead_count, drain_ahead, 0)


def body(voltages, delays, tap_sets, tap_table, weights):
    _, channels, parts, antennas, time_len = voltages.shape
    beams = weights.shape[-1]
    set_count, tap_count = tap_table.shape
    n = lax.axis_size("station")
    tm_count = lax.axis_size("tm")
    rows = channels // n
    pad = MAXD + tap_count
    rows_in = parts * antennas
    fold_rows = rows_in * pad // time_len
    group = max(rows // 4, 1)
    groups = channels // group
    sizes = (channels, parts, antennas, beams, time_len, pad, group)
    bf16, f32 = jnp.bfloat16, jnp.float32
    dma = pltpu.SemaphoreType.DMA
    in_hbm = pl.BlockSpec(memory_space=pltpu.HBM)
    operands = (
        tap_sets,
        delays,
        tap_table,
        voltages.reshape(channels, rows_in, time_len),
        weights.reshape(channels, rows_in, beams),
    )
    result = pl.pallas_call(
        functools.partial(kernel, n, tm_count, sizes),
        out_shape=pltpu.VMEM((rows, 2 * beams, time_len), bf16),
        in_specs=[in_hbm] * 5,
        out_specs=pl.BlockSpec(memory_space=pltpu.VMEM),
        scratch_shapes=[
            pltpu.SMEM(tap_sets.shape, jnp.int32),
            pltpu.SMEM(delays.shape, jnp.int32),
            pltpu.VMEM((set_count, tap_count), bf16),
            pltpu.VMEM((set_count, 1, tap_count * 128), f32),
            pltpu.VMEM((time_len, time_len), jnp.int32),
            pltpu.VMEM((pad, time_len), jnp.int32),
            pltpu.VMEM((channels, rows_in, time_len), bf16),
            pltpu.VMEM((channels, rows_in, beams), bf16),
            pltpu.VMEM((channels, fold_rows, time_len), bf16),
            pltpu.VMEM((channels, fold_rows, time_len), bf16),
            pltpu.VMEM((channels, time_len, 2 * beams), bf16),
            pltpu.VMEM((channels + rows, time_len, 2 * beams), bf16),
            pltpu.VMEM((rows, time_len, 2 * beams), f32),
            dma((3,)),
            dma((groups,)),
            dma((groups,)),
            dma((channels,)),
            dma((channels,)),
            dma((channels,)),
            dma((channels + rows,)),
            dma((group,)),
            dma((group,)),
        ],
        compiler_params=pltpu.CompilerParams(
            collective_id=0, has_side_effects=True, vmem_limit_bytes=40 * 1024 * 1024
        ),
    )(*(x if x.ndim == 1 else pltpu.with_memory_space_constraint(x, pltpu.HBM) for x in operands))
    return result.reshape(rows, 2, beams, time_len)


def solution(mesh):
    return jax.shard_map(
        body,
        mesh=mesh,
        in_specs=(
            P(("group", "station"), "chan", None, None, "tm"),
            P(("group", "station")),
            P(("group", "station"), "chan"),
            P(),
            P(("group", "station"), "chan", None, None, None),
        ),
        out_specs=P(("group", "chan", "station"), None, None, "tm"),
        check_vma=False,
    )
```

```python
import functools

import jax
import jax.numpy as jnp
from jax import lax
from jax.experimental import pallas as pl
from jax.experimental.pallas import tpu as pltpu
from jax.sharding import PartitionSpec as P

MAXD = 16
MESH = pl.DeviceIdType.MESH
LEAD = 8
LAG = 12


def kernel(
    n, tm_count, sizes, sets_hbm, delays_hbm, taps_hbm, v_hbm, w_hbm, out_buf,
    sets, delays, taps, spread, own_lag, rim_lag, v_buf, w_buf, halo_out, halo_in,
    acc_out, acc_in, own,
    small_sem, load_sem, hs_sem, hr_sem, as_sem, ar_sem,
):
    channels, parts, antennas, beams, time_len, pad, group = sizes
    rows = channels // n
    rows_in = parts * antennas
    folds = time_len // pad
    fold_rows = rows_in // folds
    set_count, tap_count = taps.shape
    head = group if n > 2 else 0
    bf16, f32 = jnp.bfloat16, jnp.float32

    me = lax.axis_index("station")
    tm = lax.axis_index("tm")
    later, earlier = lax.rem(tm + 1, tm_count), lax.rem(tm + tm_count - 1, tm_count)

    flip = jnp.where(me >= n // 2, 1, 0)
    place = me + flip * (n - 1 - 2 * me)
    ahead_dir, back_dir = flip, 1 - flip
    ahead_count = (n - 1 - place) * rows
    back_count = (place + 1) * rows
    offset = LAG + ahead_count - back_count
    start = jnp.where(place == 0, head, 0)
    single_from = jnp.where(place < n // 2 - 1, ahead_count - group, ahead_count)
    shared = (channels + rows) // group

    def channel_of(station, k):
        return (station + flip * (n - 1 - 2 * station)) * rows + k

    def ahead_channel(i):
        return channel_of(n - 1 - i // rows, lax.rem(i, rows))

    def back_channel(j):
        return channel_of(j // rows, lax.rem(j, rows))

    def load(first, count, sems):
        span = pl.ds(first, count)
        return (
            pltpu.make_async_copy(v_hbm.at[span], v_buf.at[span], load_sem.at[sems]),
            pltpu.make_async_copy(w_hbm.at[span], w_buf.at[span], load_sem.at[sems + 1]),
        )

    def halo_copy(ch):
        span = pl.ds(ch, group)
        return pltpu.make_async_remote_copy(
            src_ref=halo_out.at[span],
            dst_ref=halo_in.at[span],
            send_sem=hs_sem,
            recv_sem=hr_sem.at[ch // group],
            device_id={"tm": later},
            device_id_type=MESH,
        )

    def sum_copy(ch, direction, single=False):
        target = me + 1 - 2 * direction
        final = (ch // rows == target) & (direction == 1)
        slot = jnp.where(final, channels + lax.rem(ch, rows), ch)
        return pltpu.make_async_remote_copy(
            src_ref=acc_out.at[ch],
            dst_ref=acc_in.at[slot],
            send_sem=as_sem,
            recv_sem=ar_sem.at[jnp.where(single, shared + lax.rem(ch, group), slot // group)],
            device_id={"station": target},
            device_id_type=MESH,
        )

    def arrival(ch, direction):
        final = (ch // rows == me) & (direction == 1)
        return jnp.where(final, channels + lax.rem(ch, rows), ch)

    def wait_group(slot):
        span = acc_in.at[pl.ds(slot, group)]
        pltpu.make_async_copy(span, span, ar_sem.at[slot // group]).wait()

    def wait_single(slot):
        sem = ar_sem.at[shared + lax.rem(slot, group)]
        pltpu.make_async_copy(acc_in.at[slot], acc_in.at[slot], sem).wait()

    late_rows, early_rows = pl.ds(pad, time_len - pad), pl.ds(0, pad)

    def piece_copy(i, piece):
        ch = ahead_channel(i)
        return pltpu.make_async_remote_copy(
            src_ref=acc_out.at[ch, piece],
            dst_ref=acc_in.at[ch, piece],
            send_sem=as_sem,
            recv_sem=ar_sem.at[ch // group],
            device_id={"station": me + 1 - 2 * ahead_dir},
            device_id_type=MESH,
        )

    small = [
        pltpu.make_async_copy(taps_hbm, taps, small_sem.at[0]),
        pltpu.make_async_copy(delays_hbm, delays, small_sem.at[1]),
        pltpu.make_async_copy(sets_hbm, sets, small_sem.at[2]),
    ]
    first = ahead_channel(0)
    first_loads = load(first, group, 0)
    for copy in first_loads:
        copy.start()
    for copy in small:
        copy.start()

    barrier = pltpu.get_barrier_semaphore()

    @pl.when(me > 0)
    def _():
        pl.semaphore_signal(barrier, inc=1, device_id={"station": me - 1}, device_id_type=MESH)

    @pl.when(me < n - 1)
    def _():
        pl.semaphore_signal(barrier, inc=1, device_id={"station": me + 1}, device_id_type=MESH)

    for target in ({"tm": earlier}, {"tm": later}):
        pl.semaphore_signal(barrier, inc=1, device_id=target, device_id_type=MESH)

    for copy in load(first + group, rows - group, 2):
        copy.start()

    def load_rest(station, carry):
        for copy in load(channel_of(station, 0), rows, 2):
            copy.start()
        return carry

    lax.fori_loop(0, n - 1, load_rest, 0)

    from_row = lax.broadcasted_iota(jnp.int32, (folds * time_len, time_len), 0)
    to_lane = lax.broadcasted_iota(jnp.int32, (folds * time_len, time_len), 1)
    wanted = (to_lane // pad) * time_len + lax.rem(to_lane, pad) + time_len - pad
    picker = (from_row == wanted).astype(f32).astype(bf16)

    for copy in small:
        copy.wait()

    pick_tap = lax.broadcasted_iota(jnp.int32, (tap_count, tap_count * 128), 1) // 128
    tap_row = lax.broadcasted_iota(jnp.int32, (tap_count, tap_count * 128), 0)
    chosen = (pick_tap == tap_row).astype(f32).astype(bf16)
    values = jnp.dot(taps[...], chosen, preferred_element_type=f32)
    for m in range(set_count):
        spread[m] = values[m:m + 1]

    out_pos = lax.broadcasted_iota(jnp.int32, (time_len, time_len), 0)
    in_pos = lax.broadcasted_iota(jnp.int32, (time_len, time_len), 1)
    own_lag[...] = out_pos - in_pos - delays[0]
    rim_out = lax.broadcasted_iota(jnp.int32, (pad, time_len), 0)
    rim_in = lax.rem(lax.broadcasted_iota(jnp.int32, (pad, time_len), 1), pad) - pad
    rim_lag[...] = jnp.where(tm > 0, rim_out - rim_in - delays[0], -1)

    fold_lane = lax.broadcasted_iota(jnp.int32, (fold_rows, time_len), 1) // pad

    def toeplitz(m, lag):
        values = jnp.zeros(lag.shape, f32)
        for k in range(tap_count):
            values = jnp.where(lag == k, spread[m, :, pl.ds(k * 128, 128)], values)
        return values.astype(bf16)

    def rims_of(ch):
        rim = halo_in[ch]
        return jnp.concatenate(
            [jnp.where(fold_lane == q, rim, jnp.zeros_like(rim)) for q in range(folds)], axis=0
        )

    def filtered(filt, window):
        return lax.dot_general(
            filt, window, (((1,), (1,)), ((), ())), preferred_element_type=f32
        ).astype(bf16)

    def steered(ch, delayed):
        wr = w_buf[ch, pl.ds(0, antennas), :]
        wi = w_buf[ch, pl.ds(antennas, antennas), :]
        steer = jnp.concatenate(
            [jnp.concatenate([wr, wi], axis=1), jnp.concatenate([-wi, wr], axis=1)], axis=0
        )
        return jnp.dot(delayed, steer, preferred_element_type=f32)

    def beams_of(ch):
        @pl.when(lax.rem(ch, group) == 0)
        def _():
            halo_copy(ch).wait_recv()

        m = sets[0, ch]
        rim = toeplitz(m, rim_lag[...])
        rim = jnp.concatenate([rim, jnp.zeros((time_len - pad, time_len), bf16)], axis=0)
        filt = jnp.concatenate([toeplitz(m, own_lag[...]), rim], axis=1)
        window = jnp.concatenate([v_buf[ch], rims_of(ch)], axis=1)
        return steered(ch, filtered(filt, window))

    def pack(ch):
        wide = jnp.concatenate(
            [v_buf[ch, pl.ds(q * fold_rows, fold_rows), :] for q in range(folds)], axis=1
        )
        halo_out[ch] = jnp.dot(wide, picker, preferred_element_type=f32).astype(bf16)

        @pl.when(lax.rem(ch, group) == group - 1)
        def _():
            halo_copy(ch - (group - 1)).start()

    def late_rows_of(i):
        ch = ahead_channel(i)
        filt = toeplitz(sets[0, ch], own_lag[late_rows, :])
        total = steered(ch, filtered(filt, v_buf[ch]))
        acc_out[ch, late_rows, :] = total.astype(bf16)

    for copy in first_loads:
        copy.wait()

    if head:
        @pl.when(place == 0)
        def _():
            late_rows_of(0)

    present = 2 + jnp.where(me > 0, 1, 0) + jnp.where(me < n - 1, 1, 0)
    pl.semaphore_wait(barrier, present)

    if head:
        @pl.when(place == 0)
        def _():
            piece_copy(0, late_rows).start()

            def send_late(i, carry):
                late_rows_of(i)
                piece_copy(i, late_rows).start()
                return carry

            lax.fori_loop(1, head, send_late, 0)

            def pack_head(i, carry):
                pack(ahead_channel(i))
                return carry

            lax.fori_loop(0, head, pack_head, 0)

    for copy in load(0, channels - group, 2):
        copy.wait()

    def pack_first(i, carry):
        pack(ahead_channel(i))
        return carry

    lax.fori_loop(start, start + LEAD, pack_first, 0)

    if head:
        @pl.when(place == 0)
        def _():
            def send_early(i, carry):
                ch = ahead_channel(i)

                @pl.when(i == 0)
                def _():
                    halo_copy(ch).wait_recv()

                m = sets[0, ch]
                filt = jnp.concatenate(
                    [toeplitz(m, own_lag[early_rows, :]), toeplitz(m, rim_lag[...])], axis=1
                )
                window = jnp.concatenate([v_buf[ch], rims_of(ch)], axis=1)
                total = steered(ch, filtered(filt, window))
                acc_out[ch, early_rows, :] = total.astype(bf16)
                piece_copy(i, early_rows).start()
                return carry

            lax.fori_loop(0, head, send_early, 0)

    def step(i, carry):
        j = i - offset

        @pl.when(i + LEAD < ahead_count)
        def _():
            pack(ahead_channel(i + LEAD))

        @pl.when((j + LEAD >= 0) & (j + LEAD < back_count))
        def _():
            pack(back_channel(j + LEAD))

        @pl.when(i < ahead_count)
        def _():
            ch = ahead_channel(i)
            total = beams_of(ch)

            @pl.when(place > 0)
            def _():
                @pl.when(lax.rem(i, group) == 0)
                def _():
                    wait_group(ch)

                acc_out[ch] = (total + acc_in[ch].astype(f32)).astype(bf16)

            @pl.when(place == 0)
            def _():
                acc_out[ch] = total.astype(bf16)

            sum_copy(ch, ahead_dir, i >= single_from).start()

        @pl.when((j >= 0) & (j < back_count))
        def _():
            ch = back_channel(j)
            total = beams_of(ch)
            slot = arrival(ch, back_dir)

            @pl.when(lax.rem(j, group) == 0)
            def _():
                wait_group(slot)

            total = total + acc_in[slot].astype(f32)

            @pl.when(j < place * rows)
            def _():
                acc_out[ch] = total.astype(bf16)
                sum_copy(ch, back_dir).start()

            @pl.when(j >= place * rows)
            def _():
                own[lax.rem(j, rows)] = total

        return carry

    lax.fori_loop(start, ahead_count + LAG, step, 0)

    def drain():
        pltpu.make_async_remote_copy(
            src_ref=halo_out,
            dst_ref=halo_in,
            send_sem=hs_sem,
            recv_sem=hr_sem.at[0],
            device_id={"tm": later},
            device_id_type=MESH,
        ).wait_send()
        sent = pl.ds(0, (n - 1) * rows)
        pltpu.make_async_remote_copy(
            src_ref=acc_out.at[sent],
            dst_ref=acc_in.at[sent],
            send_sem=as_sem,
            recv_sem=ar_sem.at[0],
            device_id={"tm": later},
            device_id_type=MESH,
        ).wait_send()

    @pl.when(place > 0)
    def _():
        drain()

        def finish(k, carry):
            slot = arrival(me * rows + k, ahead_dir)
            single = k >= rows - group

            @pl.when(single)
            def _():
                wait_single(slot)

            @pl.when(jnp.logical_not(single) & (lax.rem(k, group) == 0))
            def _():
                wait_group(slot)

            out_buf[k] = (own[k] + acc_in[slot].astype(f32)).T.astype(bf16)
            return carry

        lax.fori_loop(0, rows, finish, 0)

    @pl.when(place == 0)
    def _():
        def finish(k, carry):
            out_buf[k] = own[k].T.astype(bf16)
            return carry

        lax.fori_loop(0, rows, finish, 0)
        drain()


def body(voltages, delays, tap_sets, tap_table, weights):
    _, channels, parts, antennas, time_len = voltages.shape
    beams = weights.shape[-1]
    set_count, tap_count = tap_table.shape
    n = lax.axis_size("station")
    tm_count = lax.axis_size("tm")
    rows = channels // n
    pad = MAXD + tap_count
    rows_in = parts * antennas
    fold_rows = rows_in * pad // time_len
    group = max(rows // 4, 1)
    sizes = (channels, parts, antennas, beams, time_len, pad, group)
    bf16, f32 = jnp.bfloat16, jnp.float32
    dma = pltpu.SemaphoreType.DMA
    in_hbm = pl.BlockSpec(memory_space=pltpu.HBM)
    operands = (
        tap_sets,
        delays,
        tap_table,
        voltages.reshape(channels, rows_in, time_len),
        weights.reshape(channels, rows_in, beams),
    )
    result = pl.pallas_call(
        functools.partial(kernel, n, tm_count, sizes),
        out_shape=pltpu.VMEM((rows, 2 * beams, time_len), bf16),
        in_specs=[in_hbm] * 5,
        out_specs=pl.BlockSpec(memory_space=pltpu.VMEM),
        scratch_shapes=[
            pltpu.SMEM(tap_sets.shape, jnp.int32),
            pltpu.SMEM(delays.shape, jnp.int32),
            pltpu.VMEM((set_count, tap_count), bf16),
            pltpu.VMEM((set_count, 1, tap_count * 128), f32),
            pltpu.VMEM((time_len, time_len), jnp.int32),
            pltpu.VMEM((pad, time_len), jnp.int32),
            pltpu.VMEM((channels, rows_in, time_len), bf16),
            pltpu.VMEM((channels, rows_in, beams), bf16),
            pltpu.VMEM((channels, fold_rows, time_len), bf16),
            pltpu.VMEM((channels, fold_rows, time_len), bf16),
            pltpu.VMEM((channels, time_len, 2 * beams), bf16),
            pltpu.VMEM((channels + rows, time_len, 2 * beams), bf16),
            pltpu.VMEM((rows, time_len, 2 * beams), f32),
            dma((3,)),
            dma((4,)),
            dma(()),
            dma((channels // group,)),
            dma(()),
            dma(((channels + rows) // group + group,)),
        ],
        compiler_params=pltpu.CompilerParams(
            collective_id=0, has_side_effects=True, vmem_limit_bytes=40 * 1024 * 1024
        ),
    )(*(x if x.ndim == 1 else pltpu.with_memory_space_constraint(x, pltpu.HBM) for x in operands))
    return result.reshape(rows, 2, beams, time_len)


def solution(mesh):
    return jax.shard_map(
        body,
        mesh=mesh,
        in_specs=(
            P(("group", "station"), "chan", None, None, "tm"),
            P(("group", "station")),
            P(("group", "station"), "chan"),
            P(),
            P(("group", "station"), "chan", None, None, None),
        ),
        out_specs=P(("group", "chan", "station"), None, None, "tm"),
        check_vma=False,
    )
```

```python
import functools

import jax
import jax.numpy as jnp
from jax import lax
from jax.experimental import pallas as pl
from jax.experimental.pallas import tpu as pltpu
from jax.sharding import PartitionSpec as P

MAXD = 16
MESH = pl.DeviceIdType.MESH
LEAD = 12
LAG = 12


def kernel(
    n, tm_count, sizes, sets_hbm, delays_hbm, taps_hbm, v_hbm, w_hbm, out_buf,
    sets, delays, taps, spread, own_lag, rim_lag, v_buf, w_buf, halo_out, halo_in,
    acc_out, acc_in, own,
    small_sem, load_sem, hs_sem, hr_sem, as_sem, ar_sem,
):
    channels, parts, antennas, beams, time_len, pad, group = sizes
    rows = channels // n
    rows_in = parts * antennas
    folds = time_len // pad
    fold_rows = rows_in // folds
    set_count, tap_count = taps.shape
    head = 2 * group if n > 2 else 0
    bf16, f32 = jnp.bfloat16, jnp.float32

    me = lax.axis_index("station")
    tm = lax.axis_index("tm")
    later, earlier = lax.rem(tm + 1, tm_count), lax.rem(tm + tm_count - 1, tm_count)

    flip = jnp.where(me >= n // 2, 1, 0)
    place = me + flip * (n - 1 - 2 * me)
    ahead_dir, back_dir = flip, 1 - flip
    ahead_count = (n - 1 - place) * rows
    back_count = (place + 1) * rows
    offset = LAG + ahead_count - back_count
    start = jnp.where(place == 0, head, 0)
    single_from = jnp.where(place < n // 2 - 1, ahead_count - group, ahead_count)
    shared = (channels + rows) // group

    def channel_of(station, k):
        return (station + flip * (n - 1 - 2 * station)) * rows + k

    def ahead_channel(i):
        return channel_of(n - 1 - i // rows, lax.rem(i, rows))

    def back_channel(j):
        return channel_of(j // rows, lax.rem(j, rows))

    def load(first, count, sems):
        span = pl.ds(first, count)
        return (
            pltpu.make_async_copy(v_hbm.at[span], v_buf.at[span], load_sem.at[sems]),
            pltpu.make_async_copy(w_hbm.at[span], w_buf.at[span], load_sem.at[sems + 1]),
        )

    def halo_copy(ch):
        span = pl.ds(ch, group)
        return pltpu.make_async_remote_copy(
            src_ref=halo_out.at[span],
            dst_ref=halo_in.at[span],
            send_sem=hs_sem,
            recv_sem=hr_sem.at[ch // group],
            device_id={"tm": later},
            device_id_type=MESH,
        )

    def sum_copy(ch, direction, single=False):
        target = me + 1 - 2 * direction
        final = (ch // rows == target) & (direction == 1)
        slot = jnp.where(final, channels + lax.rem(ch, rows), ch)
        return pltpu.make_async_remote_copy(
            src_ref=acc_out.at[ch],
            dst_ref=acc_in.at[slot],
            send_sem=as_sem,
            recv_sem=ar_sem.at[jnp.where(single, shared + lax.rem(ch, group), slot // group)],
            device_id={"station": target},
            device_id_type=MESH,
        )

    def arrival(ch, direction):
        final = (ch // rows == me) & (direction == 1)
        return jnp.where(final, channels + lax.rem(ch, rows), ch)

    def wait_group(slot):
        span = acc_in.at[pl.ds(slot, group)]
        pltpu.make_async_copy(span, span, ar_sem.at[slot // group]).wait()

    def wait_single(slot):
        sem = ar_sem.at[shared + lax.rem(slot, group)]
        pltpu.make_async_copy(acc_in.at[slot], acc_in.at[slot], sem).wait()

    late_rows, early_rows = pl.ds(pad, time_len - pad), pl.ds(0, pad)

    def piece_copy(i, piece):
        ch = ahead_channel(i)
        return pltpu.make_async_remote_copy(
            src_ref=acc_out.at[ch, piece],
            dst_ref=acc_in.at[ch, piece],
            send_sem=as_sem,
            recv_sem=ar_sem.at[ch // group],
            device_id={"station": me + 1 - 2 * ahead_dir},
            device_id_type=MESH,
        )

    small = [
        pltpu.make_async_copy(taps_hbm, taps, small_sem.at[0]),
        pltpu.make_async_copy(delays_hbm, delays, small_sem.at[1]),
        pltpu.make_async_copy(sets_hbm, sets, small_sem.at[2]),
    ]
    first = ahead_channel(0)
    first_loads = load(first, max(head, group), 0)
    for copy in first_loads:
        copy.start()
    for copy in small:
        copy.start()

    barrier = pltpu.get_barrier_semaphore()

    @pl.when(me > 0)
    def _():
        pl.semaphore_signal(barrier, inc=1, device_id={"station": me - 1}, device_id_type=MESH)

    @pl.when(me < n - 1)
    def _():
        pl.semaphore_signal(barrier, inc=1, device_id={"station": me + 1}, device_id_type=MESH)

    for target in ({"tm": earlier}, {"tm": later}):
        pl.semaphore_signal(barrier, inc=1, device_id=target, device_id_type=MESH)

    for copy in load(first + max(head, group), rows - max(head, group), 2):
        copy.start()

    def load_rest(station, carry):
        for copy in load(channel_of(station, 0), rows, 2):
            copy.start()
        return carry

    lax.fori_loop(0, n - 1, load_rest, 0)

    from_row = lax.broadcasted_iota(jnp.int32, (folds * time_len, time_len), 0)
    to_lane = lax.broadcasted_iota(jnp.int32, (folds * time_len, time_len), 1)
    wanted = (to_lane // pad) * time_len + lax.rem(to_lane, pad) + time_len - pad
    picker = (from_row == wanted).astype(f32).astype(bf16)

    for copy in small:
        copy.wait()

    pick_tap = lax.broadcasted_iota(jnp.int32, (tap_count, tap_count * 128), 1) // 128
    tap_row = lax.broadcasted_iota(jnp.int32, (tap_count, tap_count * 128), 0)
    chosen = (pick_tap == tap_row).astype(f32).astype(bf16)
    values = jnp.dot(taps[...], chosen, preferred_element_type=f32)
    for m in range(set_count):
        spread[m] = values[m:m + 1]

    out_pos = lax.broadcasted_iota(jnp.int32, (time_len, time_len), 0)
    in_pos = lax.broadcasted_iota(jnp.int32, (time_len, time_len), 1)
    own_lag[...] = out_pos - in_pos - delays[0]
    rim_out = lax.broadcasted_iota(jnp.int32, (pad, time_len), 0)
    rim_in = lax.rem(lax.broadcasted_iota(jnp.int32, (pad, time_len), 1), pad) - pad
    rim_lag[...] = jnp.where(tm > 0, rim_out - rim_in - delays[0], -1)

    fold_lane = lax.broadcasted_iota(jnp.int32, (fold_rows, time_len), 1) // pad

    def toeplitz(m, lag):
        values = jnp.zeros(lag.shape, f32)
        for k in range(tap_count):
            values = jnp.where(lag == k, spread[m, :, pl.ds(k * 128, 128)], values)
        return values.astype(bf16)

    def rims_of(ch):
        rim = halo_in[ch]
        return jnp.concatenate(
            [jnp.where(fold_lane == q, rim, jnp.zeros_like(rim)) for q in range(folds)], axis=0
        )

    def filtered(filt, window):
        return lax.dot_general(
            filt, window, (((1,), (1,)), ((), ())), preferred_element_type=f32
        ).astype(bf16)

    def steered(ch, delayed):
        wr = w_buf[ch, pl.ds(0, antennas), :]
        wi = w_buf[ch, pl.ds(antennas, antennas), :]
        steer = jnp.concatenate(
            [jnp.concatenate([wr, wi], axis=1), jnp.concatenate([-wi, wr], axis=1)], axis=0
        )
        return jnp.dot(delayed, steer, preferred_element_type=f32)

    def beams_of(ch):
        @pl.when(lax.rem(ch, group) == 0)
        def _():
            halo_copy(ch).wait_recv()

        m = sets[0, ch]
        rim = toeplitz(m, rim_lag[...])
        rim = jnp.concatenate([rim, jnp.zeros((time_len - pad, time_len), bf16)], axis=0)
        filt = jnp.concatenate([toeplitz(m, own_lag[...]), rim], axis=1)
        window = jnp.concatenate([v_buf[ch], rims_of(ch)], axis=1)
        return steered(ch, filtered(filt, window))

    def pack(ch):
        wide = jnp.concatenate(
            [v_buf[ch, pl.ds(q * fold_rows, fold_rows), :] for q in range(folds)], axis=1
        )
        halo_out[ch] = jnp.dot(wide, picker, preferred_element_type=f32).astype(bf16)

        @pl.when(lax.rem(ch, group) == group - 1)
        def _():
            halo_copy(ch - (group - 1)).start()

    def late_rows_of(i):
        ch = ahead_channel(i)
        filt = toeplitz(sets[0, ch], own_lag[late_rows, :])
        total = steered(ch, filtered(filt, v_buf[ch]))
        acc_out[ch, late_rows, :] = total.astype(bf16)

    for copy in first_loads:
        copy.wait()

    if head:
        @pl.when(place == 0)
        def _():
            late_rows_of(0)

    present = 2 + jnp.where(me > 0, 1, 0) + jnp.where(me < n - 1, 1, 0)
    pl.semaphore_wait(barrier, present)

    if head:
        @pl.when(place == 0)
        def _():
            piece_copy(0, late_rows).start()

            def send_late(i, carry):
                late_rows_of(i)
                piece_copy(i, late_rows).start()
                return carry

            lax.fori_loop(1, head, send_late, 0)

            def pack_head(i, carry):
                pack(ahead_channel(i))
                return carry

            lax.fori_loop(0, head, pack_head, 0)

    for copy in load(0, channels - max(head, group), 2):
        copy.wait()

    def pack_first(i, carry):
        pack(ahead_channel(i))
        return carry

    lax.fori_loop(start, start + LEAD, pack_first, 0)

    if head:
        @pl.when(place == 0)
        def _():
            def send_early(i, carry):
                ch = ahead_channel(i)

                @pl.when(lax.rem(i, group) == 0)
                def _():
                    halo_copy(ch).wait_recv()

                m = sets[0, ch]
                filt = jnp.concatenate(
                    [toeplitz(m, own_lag[early_rows, :]), toeplitz(m, rim_lag[...])], axis=1
                )
                window = jnp.concatenate([v_buf[ch], rims_of(ch)], axis=1)
                total = steered(ch, filtered(filt, window))
                acc_out[ch, early_rows, :] = total.astype(bf16)
                piece_copy(i, early_rows).start()
                return carry

            lax.fori_loop(0, head, send_early, 0)

    def step(i, carry):
        j = i - offset

        @pl.when(i + LEAD < ahead_count)
        def _():
            pack(ahead_channel(i + LEAD))

        @pl.when((j + LEAD >= 0) & (j + LEAD < back_count))
        def _():
            pack(back_channel(j + LEAD))

        @pl.when(i < ahead_count)
        def _():
            ch = ahead_channel(i)
            total = beams_of(ch)

            @pl.when(place > 0)
            def _():
                @pl.when(lax.rem(i, group) == 0)
                def _():
                    wait_group(ch)

                acc_out[ch] = (total + acc_in[ch].astype(f32)).astype(bf16)

            @pl.when(place == 0)
            def _():
                acc_out[ch] = total.astype(bf16)

            sum_copy(ch, ahead_dir, i >= single_from).start()

        @pl.when((j >= 0) & (j < back_count))
        def _():
            ch = back_channel(j)
            total = beams_of(ch)
            slot = arrival(ch, back_dir)

            @pl.when(lax.rem(j, group) == 0)
            def _():
                wait_group(slot)

            total = total + acc_in[slot].astype(f32)

            @pl.when(j < place * rows)
            def _():
                acc_out[ch] = total.astype(bf16)
                sum_copy(ch, back_dir).start()

            @pl.when(j >= place * rows)
            def _():
                own[lax.rem(j, rows)] = total

        return carry

    lax.fori_loop(start, ahead_count + LAG, step, 0)

    def drain():
        pltpu.make_async_remote_copy(
            src_ref=halo_out,
            dst_ref=halo_in,
            send_sem=hs_sem,
            recv_sem=hr_sem.at[0],
            device_id={"tm": later},
            device_id_type=MESH,
        ).wait_send()
        sent = pl.ds(0, (n - 1) * rows)
        pltpu.make_async_remote_copy(
            src_ref=acc_out.at[sent],
            dst_ref=acc_in.at[sent],
            send_sem=as_sem,
            recv_sem=ar_sem.at[0],
            device_id={"tm": later},
            device_id_type=MESH,
        ).wait_send()

    @pl.when(place > 0)
    def _():
        drain()

        def finish(k, carry):
            slot = arrival(me * rows + k, ahead_dir)
            single = k >= rows - group

            @pl.when(single)
            def _():
                wait_single(slot)

            @pl.when(jnp.logical_not(single) & (lax.rem(k, group) == 0))
            def _():
                wait_group(slot)

            out_buf[k] = (own[k] + acc_in[slot].astype(f32)).T.astype(bf16)
            return carry

        lax.fori_loop(0, rows, finish, 0)

    @pl.when(place == 0)
    def _():
        def finish(k, carry):
            out_buf[k] = own[k].T.astype(bf16)
            return carry

        lax.fori_loop(0, rows, finish, 0)
        drain()


def body(voltages, delays, tap_sets, tap_table, weights):
    _, channels, parts, antennas, time_len = voltages.shape
    beams = weights.shape[-1]
    set_count, tap_count = tap_table.shape
    n = lax.axis_size("station")
    tm_count = lax.axis_size("tm")
    rows = channels // n
    pad = MAXD + tap_count
    rows_in = parts * antennas
    fold_rows = rows_in * pad // time_len
    group = max(rows // 4, 1)
    sizes = (channels, parts, antennas, beams, time_len, pad, group)
    bf16, f32 = jnp.bfloat16, jnp.float32
    dma = pltpu.SemaphoreType.DMA
    in_hbm = pl.BlockSpec(memory_space=pltpu.HBM)
    operands = (
        tap_sets,
        delays,
        tap_table,
        voltages.reshape(channels, rows_in, time_len),
        weights.reshape(channels, rows_in, beams),
    )
    result = pl.pallas_call(
        functools.partial(kernel, n, tm_count, sizes),
        out_shape=pltpu.VMEM((rows, 2 * beams, time_len), bf16),
        in_specs=[in_hbm] * 5,
        out_specs=pl.BlockSpec(memory_space=pltpu.VMEM),
        scratch_shapes=[
            pltpu.SMEM(tap_sets.shape, jnp.int32),
            pltpu.SMEM(delays.shape, jnp.int32),
            pltpu.VMEM((set_count, tap_count), bf16),
            pltpu.VMEM((set_count, 1, tap_count * 128), f32),
            pltpu.VMEM((time_len, time_len), jnp.int32),
            pltpu.VMEM((pad, time_len), jnp.int32),
            pltpu.VMEM((channels, rows_in, time_len), bf16),
            pltpu.VMEM((channels, rows_in, beams), bf16),
            pltpu.VMEM((channels, fold_rows, time_len), bf16),
            pltpu.VMEM((channels, fold_rows, time_len), bf16),
            pltpu.VMEM((channels, time_len, 2 * beams), bf16),
            pltpu.VMEM((channels + rows, time_len, 2 * beams), bf16),
            pltpu.VMEM((rows, time_len, 2 * beams), f32),
            dma((3,)),
            dma((4,)),
            dma(()),
            dma((channels // group,)),
            dma(()),
            dma(((channels + rows) // group + group,)),
        ],
        compiler_params=pltpu.CompilerParams(
            collective_id=0, has_side_effects=True, vmem_limit_bytes=40 * 1024 * 1024
        ),
    )(*(x if x.ndim == 1 else pltpu.with_memory_space_constraint(x, pltpu.HBM) for x in operands))
    return result.reshape(rows, 2, beams, time_len)


def solution(mesh):
    return jax.shard_map(
        body,
        mesh=mesh,
        in_specs=(
            P(("group", "station"), "chan", None, None, "tm"),
            P(("group", "station")),
            P(("group", "station"), "chan"),
            P(),
            P(("group", "station"), "chan", None, None, None),
        ),
        out_specs=P(("group", "chan", "station"), None, None, "tm"),
        check_vma=False,
    )
```

```python
import functools

import jax
import jax.numpy as jnp
from jax import lax
from jax.experimental import pallas as pl
from jax.experimental.pallas import tpu as pltpu
from jax.sharding import PartitionSpec as P

MAXD = 16
MESH = pl.DeviceIdType.MESH
LEAD = 16
LAG = 16


def kernel(
    n, tm_count, sizes, sets_hbm, delays_hbm, taps_hbm, v_hbm, w_hbm, out_buf,
    sets, delays, taps, spread, own_lag, rim_lag, v_buf, w_buf, halo_out, halo_in,
    acc_out, acc_in, own,
    small_sem, load_sem, hs_sem, hr_sem, as_sem, ar_sem,
):
    channels, parts, antennas, beams, time_len, pad, group = sizes
    rows = channels // n
    rows_in = parts * antennas
    folds = time_len // pad
    fold_rows = rows_in // folds
    set_count, tap_count = taps.shape
    head = group if n > 2 else 0
    tail = max(group // 2, 1)
    bf16, f32 = jnp.bfloat16, jnp.float32

    me = lax.axis_index("station")
    tm = lax.axis_index("tm")
    later, earlier = lax.rem(tm + 1, tm_count), lax.rem(tm + tm_count - 1, tm_count)

    flip = jnp.where(me >= n // 2, 1, 0)
    place = me + flip * (n - 1 - 2 * me)
    ahead_dir, back_dir = flip, 1 - flip
    ahead_count = (n - 1 - place) * rows
    back_count = (place + 1) * rows
    offset = LAG + ahead_count - back_count
    start = jnp.where(place == 0, head, 0)
    single_from = jnp.where(place < n // 2 - 1, ahead_count - tail, ahead_count)
    shared = (channels + rows) // group

    def channel_of(station, k):
        return (station + flip * (n - 1 - 2 * station)) * rows + k

    def ahead_channel(i):
        return channel_of(n - 1 - i // rows, lax.rem(i, rows))

    def back_channel(j):
        return channel_of(j // rows, lax.rem(j, rows))

    def load(first, count, sems):
        span = pl.ds(first, count)
        return (
            pltpu.make_async_copy(v_hbm.at[span], v_buf.at[span], load_sem.at[sems]),
            pltpu.make_async_copy(w_hbm.at[span], w_buf.at[span], load_sem.at[sems + 1]),
        )

    def halo_copy(ch):
        span = pl.ds(ch, group)
        return pltpu.make_async_remote_copy(
            src_ref=halo_out.at[span],
            dst_ref=halo_in.at[span],
            send_sem=hs_sem,
            recv_sem=hr_sem.at[ch // group],
            device_id={"tm": later},
            device_id_type=MESH,
        )

    def sum_copy(ch, direction, single=False):
        target = me + 1 - 2 * direction
        final = (ch // rows == target) & (direction == 1)
        slot = jnp.where(final, channels + lax.rem(ch, rows), ch)
        return pltpu.make_async_remote_copy(
            src_ref=acc_out.at[ch],
            dst_ref=acc_in.at[slot],
            send_sem=as_sem,
            recv_sem=ar_sem.at[jnp.where(single, shared + lax.rem(ch, tail), slot // group)],
            device_id={"station": target},
            device_id_type=MESH,
        )

    def arrival(ch, direction):
        final = (ch // rows == me) & (direction == 1)
        return jnp.where(final, channels + lax.rem(ch, rows), ch)

    def wait_group(slot, count=group):
        span = acc_in.at[pl.ds(slot, count)]
        pltpu.make_async_copy(span, span, ar_sem.at[slot // group]).wait()

    def wait_single(slot):
        sem = ar_sem.at[shared + lax.rem(slot, tail)]
        pltpu.make_async_copy(acc_in.at[slot], acc_in.at[slot], sem).wait()

    late_rows, early_rows = pl.ds(pad, time_len - pad), pl.ds(0, pad)

    def piece_copy(i, piece):
        ch = ahead_channel(i)
        return pltpu.make_async_remote_copy(
            src_ref=acc_out.at[ch, piece],
            dst_ref=acc_in.at[ch, piece],
            send_sem=as_sem,
            recv_sem=ar_sem.at[ch // group],
            device_id={"station": me + 1 - 2 * ahead_dir},
            device_id_type=MESH,
        )

    small = [
        pltpu.make_async_copy(taps_hbm, taps, small_sem.at[0]),
        pltpu.make_async_copy(delays_hbm, delays, small_sem.at[1]),
        pltpu.make_async_copy(sets_hbm, sets, small_sem.at[2]),
    ]
    first = ahead_channel(0)
    first_loads = load(first, max(head, group), 0)
    for copy in first_loads:
        copy.start()
    for copy in small:
        copy.start()

    barrier = pltpu.get_barrier_semaphore()

    @pl.when(me > 0)
    def _():
        pl.semaphore_signal(barrier, inc=1, device_id={"station": me - 1}, device_id_type=MESH)

    @pl.when(me < n - 1)
    def _():
        pl.semaphore_signal(barrier, inc=1, device_id={"station": me + 1}, device_id_type=MESH)

    for target in ({"tm": earlier}, {"tm": later}):
        pl.semaphore_signal(barrier, inc=1, device_id=target, device_id_type=MESH)

    for copy in load(first + max(head, group), rows - max(head, group), 2):
        copy.start()

    def load_rest(station, carry):
        for copy in load(channel_of(station, 0), rows, 2):
            copy.start()
        return carry

    lax.fori_loop(0, n - 1, load_rest, 0)

    from_row = lax.broadcasted_iota(jnp.int32, (folds * time_len, time_len), 0)
    to_lane = lax.broadcasted_iota(jnp.int32, (folds * time_len, time_len), 1)
    wanted = (to_lane // pad) * time_len + lax.rem(to_lane, pad) + time_len - pad
    picker = (from_row == wanted).astype(f32).astype(bf16)

    for copy in small:
        copy.wait()

    pick_tap = lax.broadcasted_iota(jnp.int32, (tap_count, tap_count * 128), 1) // 128
    tap_row = lax.broadcasted_iota(jnp.int32, (tap_count, tap_count * 128), 0)
    chosen = (pick_tap == tap_row).astype(f32).astype(bf16)
    values = jnp.dot(taps[...], chosen, preferred_element_type=f32)
    for m in range(set_count):
        spread[m] = values[m:m + 1]

    out_pos = lax.broadcasted_iota(jnp.int32, (time_len, time_len), 0)
    in_pos = lax.broadcasted_iota(jnp.int32, (time_len, time_len), 1)
    own_lag[...] = out_pos - in_pos - delays[0]
    rim_out = lax.broadcasted_iota(jnp.int32, (pad, time_len), 0)
    rim_in = lax.rem(lax.broadcasted_iota(jnp.int32, (pad, time_len), 1), pad) - pad
    rim_lag[...] = jnp.where(tm > 0, rim_out - rim_in - delays[0], -1)

    fold_lane = lax.broadcasted_iota(jnp.int32, (fold_rows, time_len), 1) // pad

    def toeplitz(m, lag):
        values = jnp.zeros(lag.shape, f32)
        for k in range(tap_count):
            values = jnp.where(lag == k, spread[m, :, pl.ds(k * 128, 128)], values)
        return values.astype(bf16)

    def rims_of(ch):
        rim = halo_in[ch]
        return jnp.concatenate(
            [jnp.where(fold_lane == q, rim, jnp.zeros_like(rim)) for q in range(folds)], axis=0
        )

    def filtered(filt, window):
        return lax.dot_general(
            filt, window, (((1,), (1,)), ((), ())), preferred_element_type=f32
        ).astype(bf16)

    def steered(ch, delayed):
        wr = w_buf[ch, pl.ds(0, antennas), :]
        wi = w_buf[ch, pl.ds(antennas, antennas), :]
        steer = jnp.concatenate(
            [jnp.concatenate([wr, wi], axis=1), jnp.concatenate([-wi, wr], axis=1)], axis=0
        )
        return jnp.dot(delayed, steer, preferred_element_type=f32)

    def beams_of(ch):
        @pl.when(lax.rem(ch, group) == 0)
        def _():
            halo_copy(ch).wait_recv()

        m = sets[0, ch]
        rim = toeplitz(m, rim_lag[...])
        rim = jnp.concatenate([rim, jnp.zeros((time_len - pad, time_len), bf16)], axis=0)
        filt = jnp.concatenate([toeplitz(m, own_lag[...]), rim], axis=1)
        window = jnp.concatenate([v_buf[ch], rims_of(ch)], axis=1)
        return steered(ch, filtered(filt, window))

    def pack(ch):
        wide = jnp.concatenate(
            [v_buf[ch, pl.ds(q * fold_rows, fold_rows), :] for q in range(folds)], axis=1
        )
        halo_out[ch] = jnp.dot(wide, picker, preferred_element_type=f32).astype(bf16)

        @pl.when(lax.rem(ch, group) == group - 1)
        def _():
            halo_copy(ch - (group - 1)).start()

    def late_rows_of(i):
        ch = ahead_channel(i)
        filt = toeplitz(sets[0, ch], own_lag[late_rows, :])
        total = steered(ch, filtered(filt, v_buf[ch]))
        acc_out[ch, late_rows, :] = total.astype(bf16)

    for copy in first_loads:
        copy.wait()

    if head:
        @pl.when(place == 0)
        def _():
            late_rows_of(0)

    present = 2 + jnp.where(me > 0, 1, 0) + jnp.where(me < n - 1, 1, 0)
    pl.semaphore_wait(barrier, present)

    if head:
        @pl.when(place == 0)
        def _():
            piece_copy(0, late_rows).start()

            def send_late(i, carry):
                late_rows_of(i)
                piece_copy(i, late_rows).start()
                return carry

            lax.fori_loop(1, head, send_late, 0)

            def pack_head(i, carry):
                pack(ahead_channel(i))
                return carry

            lax.fori_loop(0, head, pack_head, 0)

    for copy in load(0, channels - max(head, group), 2):
        copy.wait()

    def pack_first(i, carry):
        pack(ahead_channel(i))
        return carry

    lax.fori_loop(start, start + LEAD, pack_first, 0)

    if head:
        @pl.when(place == 0)
        def _():
            def send_early(i, carry):
                ch = ahead_channel(i)

                @pl.when(lax.rem(i, group) == 0)
                def _():
                    halo_copy(ch).wait_recv()

                m = sets[0, ch]
                filt = jnp.concatenate(
                    [toeplitz(m, own_lag[early_rows, :]), toeplitz(m, rim_lag[...])], axis=1
                )
                window = jnp.concatenate([v_buf[ch], rims_of(ch)], axis=1)
                total = steered(ch, filtered(filt, window))
                acc_out[ch, early_rows, :] = total.astype(bf16)
                piece_copy(i, early_rows).start()
                return carry

            lax.fori_loop(0, head, send_early, 0)

    def step(i, carry):
        j = i - offset

        @pl.when(i + LEAD < ahead_count)
        def _():
            pack(ahead_channel(i + LEAD))

        @pl.when((j + LEAD >= 0) & (j + LEAD < back_count))
        def _():
            pack(back_channel(j + LEAD))

        @pl.when(i < ahead_count)
        def _():
            ch = ahead_channel(i)
            total = beams_of(ch)

            @pl.when(place > 0)
            def _():
                @pl.when(lax.rem(i, group) == 0)
                def _():
                    wait_group(ch)

                acc_out[ch] = (total + acc_in[ch].astype(f32)).astype(bf16)

            @pl.when(place == 0)
            def _():
                acc_out[ch] = total.astype(bf16)

            sum_copy(ch, ahead_dir, i >= single_from).start()

        @pl.when((j >= 0) & (j < back_count))
        def _():
            ch = back_channel(j)
            total = beams_of(ch)
            slot = arrival(ch, back_dir)

            @pl.when(lax.rem(j, group) == 0)
            def _():
                wait_group(slot)

            total = total + acc_in[slot].astype(f32)

            @pl.when(j < place * rows)
            def _():
                acc_out[ch] = total.astype(bf16)
                sum_copy(ch, back_dir).start()

            @pl.when(j >= place * rows)
            def _():
                own[lax.rem(j, rows)] = total

        return carry

    lax.fori_loop(start, ahead_count + LAG, step, 0)

    def drain():
        pltpu.make_async_remote_copy(
            src_ref=halo_out,
            dst_ref=halo_in,
            send_sem=hs_sem,
            recv_sem=hr_sem.at[0],
            device_id={"tm": later},
            device_id_type=MESH,
        ).wait_send()
        sent = pl.ds(0, (n - 1) * rows)
        pltpu.make_async_remote_copy(
            src_ref=acc_out.at[sent],
            dst_ref=acc_in.at[sent],
            send_sem=as_sem,
            recv_sem=ar_sem.at[0],
            device_id={"tm": later},
            device_id_type=MESH,
        ).wait_send()

    @pl.when(place > 0)
    def _():
        drain()

        def finish(k, carry):
            slot = arrival(me * rows + k, ahead_dir)
            @pl.when(k >= rows - tail)
            def _():
                wait_single(slot)

            @pl.when((k < rows - group) & (lax.rem(k, group) == 0))
            def _():
                wait_group(slot)

            if group > tail:
                @pl.when(k == rows - group)
                def _():
                    wait_group(slot, group - tail)

            out_buf[k] = (own[k] + acc_in[slot].astype(f32)).T.astype(bf16)
            return carry

        lax.fori_loop(0, rows, finish, 0)

    @pl.when(place == 0)
    def _():
        def finish(k, carry):
            out_buf[k] = own[k].T.astype(bf16)
            return carry

        lax.fori_loop(0, rows, finish, 0)
        drain()


def body(voltages, delays, tap_sets, tap_table, weights):
    _, channels, parts, antennas, time_len = voltages.shape
    beams = weights.shape[-1]
    set_count, tap_count = tap_table.shape
    n = lax.axis_size("station")
    tm_count = lax.axis_size("tm")
    rows = channels // n
    pad = MAXD + tap_count
    rows_in = parts * antennas
    fold_rows = rows_in * pad // time_len
    group = max(rows // 2, 1)
    sizes = (channels, parts, antennas, beams, time_len, pad, group)
    bf16, f32 = jnp.bfloat16, jnp.float32
    dma = pltpu.SemaphoreType.DMA
    in_hbm = pl.BlockSpec(memory_space=pltpu.HBM)
    operands = (
        tap_sets,
        delays,
        tap_table,
        voltages.reshape(channels, rows_in, time_len),
        weights.reshape(channels, rows_in, beams),
    )
    result = pl.pallas_call(
        functools.partial(kernel, n, tm_count, sizes),
        out_shape=pltpu.VMEM((rows, 2 * beams, time_len), bf16),
        in_specs=[in_hbm] * 5,
        out_specs=pl.BlockSpec(memory_space=pltpu.VMEM),
        scratch_shapes=[
            pltpu.SMEM(tap_sets.shape, jnp.int32),
            pltpu.SMEM(delays.shape, jnp.int32),
            pltpu.VMEM((set_count, tap_count), bf16),
            pltpu.VMEM((set_count, 1, tap_count * 128), f32),
            pltpu.VMEM((time_len, time_len), jnp.int32),
            pltpu.VMEM((pad, time_len), jnp.int32),
            pltpu.VMEM((channels, rows_in, time_len), bf16),
            pltpu.VMEM((channels, rows_in, beams), bf16),
            pltpu.VMEM((channels, fold_rows, time_len), bf16),
            pltpu.VMEM((channels, fold_rows, time_len), bf16),
            pltpu.VMEM((channels, time_len, 2 * beams), bf16),
            pltpu.VMEM((channels + rows, time_len, 2 * beams), bf16),
            pltpu.VMEM((rows, time_len, 2 * beams), f32),
            dma((3,)),
            dma((4,)),
            dma(()),
            dma((channels // group,)),
            dma(()),
            dma(((channels + rows) // group + max(group // 2, 1),)),
        ],
        compiler_params=pltpu.CompilerParams(
            collective_id=0, has_side_effects=True, vmem_limit_bytes=40 * 1024 * 1024
        ),
    )(*(x if x.ndim == 1 else pltpu.with_memory_space_constraint(x, pltpu.HBM) for x in operands))
    return result.reshape(rows, 2, beams, time_len)


def solution(mesh):
    return jax.shard_map(
        body,
        mesh=mesh,
        in_specs=(
            P(("group", "station"), "chan", None, None, "tm"),
            P(("group", "station")),
            P(("group", "station"), "chan"),
            P(),
            P(("group", "station"), "chan", None, None, None),
        ),
        out_specs=P(("group", "chan", "station"), None, None, "tm"),
        check_vma=False,
    )
```

```python
import functools

import jax
import jax.numpy as jnp
from jax import lax
from jax.experimental import pallas as pl
from jax.experimental.pallas import tpu as pltpu
from jax.sharding import PartitionSpec as P

MAXD = 16
MESH = pl.DeviceIdType.MESH
GROUPS_AHEAD = 1
LAG = 16


def kernel(
    n, tm_count, sizes, sets_hbm, delays_hbm, taps_hbm, v_hbm, w_hbm, out_buf,
    sets, delays, taps, spread, own_lag, rim_lag, v_buf, w_buf, halo_out, halo_in,
    acc_out, acc_in, own,
    small_sem, load_sem, hs_sem, hr_sem, as_sem, ar_sem,
):
    channels, parts, antennas, beams, time_len, pad, group = sizes
    rows = channels // n
    rows_in = parts * antennas
    folds = time_len // pad
    fold_rows = rows_in // folds
    set_count, tap_count = taps.shape
    head = group if n > 2 else 0
    tail = max(group // 2, 1)
    lead = GROUPS_AHEAD * group
    bf16, f32 = jnp.bfloat16, jnp.float32

    me = lax.axis_index("station")
    tm = lax.axis_index("tm")
    later, earlier = lax.rem(tm + 1, tm_count), lax.rem(tm + tm_count - 1, tm_count)

    flip = jnp.where(me >= n // 2, 1, 0)
    place = me + flip * (n - 1 - 2 * me)
    ahead_dir, back_dir = flip, 1 - flip
    ahead_count = (n - 1 - place) * rows
    back_count = (place + 1) * rows
    offset = LAG + ahead_count - back_count
    start = jnp.where(place == 0, head, 0)
    single_from = jnp.where(place < n // 2 - 1, ahead_count - tail, ahead_count)
    shared = (channels + rows) // group

    def channel_of(station, k):
        return (station + flip * (n - 1 - 2 * station)) * rows + k

    def ahead_channel(i):
        return channel_of(n - 1 - i // rows, lax.rem(i, rows))

    def back_channel(j):
        return channel_of(j // rows, lax.rem(j, rows))

    def load(first, count, sems):
        span = pl.ds(first, count)
        return (
            pltpu.make_async_copy(v_hbm.at[span], v_buf.at[span], load_sem.at[sems]),
            pltpu.make_async_copy(w_hbm.at[span], w_buf.at[span], load_sem.at[sems + 1]),
        )

    def halo_copy(ch):
        span = pl.ds(ch, group)
        return pltpu.make_async_remote_copy(
            src_ref=halo_out.at[span],
            dst_ref=halo_in.at[span],
            send_sem=hs_sem,
            recv_sem=hr_sem.at[ch // group],
            device_id={"tm": later},
            device_id_type=MESH,
        )

    def sum_copy(ch, direction, single=False):
        target = me + 1 - 2 * direction
        final = (ch // rows == target) & (direction == 1)
        slot = jnp.where(final, channels + lax.rem(ch, rows), ch)
        return pltpu.make_async_remote_copy(
            src_ref=acc_out.at[ch],
            dst_ref=acc_in.at[slot],
            send_sem=as_sem,
            recv_sem=ar_sem.at[jnp.where(single, shared + lax.rem(ch, tail), slot // group)],
            device_id={"station": target},
            device_id_type=MESH,
        )

    def arrival(ch, direction):
        final = (ch // rows == me) & (direction == 1)
        return jnp.where(final, channels + lax.rem(ch, rows), ch)

    def wait_group(slot, count=group):
        span = acc_in.at[pl.ds(slot, count)]
        pltpu.make_async_copy(span, span, ar_sem.at[slot // group]).wait()

    def wait_single(slot):
        sem = ar_sem.at[shared + lax.rem(slot, tail)]
        pltpu.make_async_copy(acc_in.at[slot], acc_in.at[slot], sem).wait()

    late_rows, early_rows = pl.ds(pad, time_len - pad), pl.ds(0, pad)

    def piece_copy(i, piece):
        ch = ahead_channel(i)
        return pltpu.make_async_remote_copy(
            src_ref=acc_out.at[ch, piece],
            dst_ref=acc_in.at[ch, piece],
            send_sem=as_sem,
            recv_sem=ar_sem.at[ch // group],
            device_id={"station": me + 1 - 2 * ahead_dir},
            device_id_type=MESH,
        )

    small = [
        pltpu.make_async_copy(taps_hbm, taps, small_sem.at[0]),
        pltpu.make_async_copy(delays_hbm, delays, small_sem.at[1]),
        pltpu.make_async_copy(sets_hbm, sets, small_sem.at[2]),
    ]
    first = ahead_channel(0)
    first_loads, head_loads = load(first, 1, 0), load(first + 1, group - 1, 4)
    for copy in first_loads + head_loads:
        copy.start()
    for copy in small:
        copy.start()

    barrier = pltpu.get_barrier_semaphore()

    @pl.when(me > 0)
    def _():
        pl.semaphore_signal(barrier, inc=1, device_id={"station": me - 1}, device_id_type=MESH)

    @pl.when(me < n - 1)
    def _():
        pl.semaphore_signal(barrier, inc=1, device_id={"station": me + 1}, device_id_type=MESH)

    for target in ({"tm": earlier}, {"tm": later}):
        pl.semaphore_signal(barrier, inc=1, device_id=target, device_id_type=MESH)

    for copy in load(first + max(head, group), rows - max(head, group), 2):
        copy.start()

    def load_rest(station, carry):
        for copy in load(channel_of(station, 0), rows, 2):
            copy.start()
        return carry

    lax.fori_loop(0, n - 1, load_rest, 0)

    from_row = lax.broadcasted_iota(jnp.int32, (folds * time_len, time_len), 0)
    to_lane = lax.broadcasted_iota(jnp.int32, (folds * time_len, time_len), 1)
    wanted = (to_lane // pad) * time_len + lax.rem(to_lane, pad) + time_len - pad
    picker = (from_row == wanted).astype(f32).astype(bf16)

    for copy in small:
        copy.wait()

    pick_tap = lax.broadcasted_iota(jnp.int32, (tap_count, tap_count * 128), 1) // 128
    tap_row = lax.broadcasted_iota(jnp.int32, (tap_count, tap_count * 128), 0)
    chosen = (pick_tap == tap_row).astype(f32).astype(bf16)
    values = jnp.dot(taps[...], chosen, preferred_element_type=f32)
    for m in range(set_count):
        spread[m] = values[m:m + 1]

    out_pos = lax.broadcasted_iota(jnp.int32, (time_len, time_len), 0)
    in_pos = lax.broadcasted_iota(jnp.int32, (time_len, time_len), 1)
    own_lag[...] = out_pos - in_pos - delays[0]
    rim_out = lax.broadcasted_iota(jnp.int32, (pad, time_len), 0)
    rim_in = lax.rem(lax.broadcasted_iota(jnp.int32, (pad, time_len), 1), pad) - pad
    rim_lag[...] = jnp.where(tm > 0, rim_out - rim_in - delays[0], -1)

    fold_lane = lax.broadcasted_iota(jnp.int32, (fold_rows, time_len), 1) // pad

    def toeplitz(m, lag):
        values = jnp.zeros(lag.shape, f32)
        for k in range(tap_count):
            values = jnp.where(lag == k, spread[m, :, pl.ds(k * 128, 128)], values)
        return values.astype(bf16)

    def rims_of(ch):
        rim = halo_in[ch]
        return jnp.concatenate(
            [jnp.where(fold_lane == q, rim, jnp.zeros_like(rim)) for q in range(folds)], axis=0
        )

    def filtered(filt, window):
        return lax.dot_general(
            filt, window, (((1,), (1,)), ((), ())), preferred_element_type=f32
        ).astype(bf16)

    def steered(ch, delayed):
        wr = w_buf[ch, pl.ds(0, antennas), :]
        wi = w_buf[ch, pl.ds(antennas, antennas), :]
        steer = jnp.concatenate(
            [jnp.concatenate([wr, wi], axis=1), jnp.concatenate([-wi, wr], axis=1)], axis=0
        )
        return jnp.dot(delayed, steer, preferred_element_type=f32)

    def beams_of(ch):
        @pl.when(lax.rem(ch, group) == 0)
        def _():
            halo_copy(ch).wait_recv()

        m = sets[0, ch]
        rim = toeplitz(m, rim_lag[...])
        rim = jnp.concatenate([rim, jnp.zeros((time_len - pad, time_len), bf16)], axis=0)
        filt = jnp.concatenate([toeplitz(m, own_lag[...]), rim], axis=1)
        window = jnp.concatenate([v_buf[ch], rims_of(ch)], axis=1)
        return steered(ch, filtered(filt, window))

    def pack(ch):
        span = pl.ds(ch, group)
        wide = jnp.concatenate(
            [
                v_buf[span, pl.ds(q * fold_rows, fold_rows), :].reshape(group * fold_rows, time_len)
                for q in range(folds)
            ],
            axis=1,
        )
        packed = jnp.dot(wide, picker, preferred_element_type=f32).astype(bf16)
        halo_out[span] = packed.reshape(group, fold_rows, time_len)
        halo_copy(ch).start()

    def late_rows_of(i):
        ch = ahead_channel(i)
        filt = toeplitz(sets[0, ch], own_lag[late_rows, :])
        total = steered(ch, filtered(filt, v_buf[ch]))
        acc_out[ch, late_rows, :] = total.astype(bf16)

    for copy in first_loads:
        copy.wait()

    if head:
        @pl.when(place == 0)
        def _():
            late_rows_of(0)

    present = 2 + jnp.where(me > 0, 1, 0) + jnp.where(me < n - 1, 1, 0)
    pl.semaphore_wait(barrier, present)

    def send_late(i, carry):
        late_rows_of(i)
        piece_copy(i, late_rows).start()
        return carry

    if head:
        @pl.when(place == 0)
        def _():
            piece_copy(0, late_rows).start()

            for copy in head_loads:
                copy.wait()

            lax.fori_loop(1, head, send_late, 0)

            pack(first)

    @pl.when(place > 0)
    def _():
        for copy in head_loads:
            copy.wait()

    for copy in load(0, channels - max(head, group), 2):
        copy.wait()

    def pack_first(g, carry):
        pack(ahead_channel(start + g * group))
        return carry

    lax.fori_loop(0, lead // group, pack_first, 0)

    if head:
        @pl.when(place == 0)
        def _():
            def send_early(i, carry):
                ch = ahead_channel(i)

                @pl.when(lax.rem(i, group) == 0)
                def _():
                    halo_copy(ch).wait_recv()

                m = sets[0, ch]
                filt = jnp.concatenate(
                    [toeplitz(m, own_lag[early_rows, :]), toeplitz(m, rim_lag[...])], axis=1
                )
                window = jnp.concatenate([v_buf[ch], rims_of(ch)], axis=1)
                total = steered(ch, filtered(filt, window))
                acc_out[ch, early_rows, :] = total.astype(bf16)
                piece_copy(i, early_rows).start()
                return carry

            lax.fori_loop(0, head, send_early, 0)

    def step(i, carry):
        j = i - offset

        @pl.when((i + lead < ahead_count) & (lax.rem(i, group) == 0))
        def _():
            pack(ahead_channel(i + lead))

        @pl.when((j + lead >= 0) & (j + lead < back_count) & (lax.rem(j + lead, group) == 0))
        def _():
            pack(back_channel(j + lead))

        @pl.when(i < ahead_count)
        def _():
            ch = ahead_channel(i)
            total = beams_of(ch)

            @pl.when(place > 0)
            def _():
                @pl.when(lax.rem(i, group) == 0)
                def _():
                    wait_group(ch)

                acc_out[ch] = (total + acc_in[ch].astype(f32)).astype(bf16)

            @pl.when(place == 0)
            def _():
                acc_out[ch] = total.astype(bf16)

            sum_copy(ch, ahead_dir, i >= single_from).start()

        @pl.when((j >= 0) & (j < back_count))
        def _():
            ch = back_channel(j)
            total = beams_of(ch)
            slot = arrival(ch, back_dir)

            @pl.when(lax.rem(j, group) == 0)
            def _():
                wait_group(slot)

            total = total + acc_in[slot].astype(f32)

            @pl.when(j < place * rows)
            def _():
                acc_out[ch] = total.astype(bf16)
                sum_copy(ch, back_dir).start()

            @pl.when(j >= place * rows)
            def _():
                own[lax.rem(j, rows)] = total

        return carry

    lax.fori_loop(start, ahead_count + LAG, step, 0)

    def drain():
        pltpu.make_async_remote_copy(
            src_ref=halo_out,
            dst_ref=halo_in,
            send_sem=hs_sem,
            recv_sem=hr_sem.at[0],
            device_id={"tm": later},
            device_id_type=MESH,
        ).wait_send()
        sent = pl.ds(0, (n - 1) * rows)
        pltpu.make_async_remote_copy(
            src_ref=acc_out.at[sent],
            dst_ref=acc_in.at[sent],
            send_sem=as_sem,
            recv_sem=ar_sem.at[0],
            device_id={"tm": later},
            device_id_type=MESH,
        ).wait_send()

    @pl.when(place > 0)
    def _():
        drain()

        def finish(k, carry):
            slot = arrival(me * rows + k, ahead_dir)
            @pl.when(k >= rows - tail)
            def _():
                wait_single(slot)

            @pl.when((k < rows - group) & (lax.rem(k, group) == 0))
            def _():
                wait_group(slot)

            if group > tail:
                @pl.when(k == rows - group)
                def _():
                    wait_group(slot, group - tail)

            out_buf[k] = (own[k] + acc_in[slot].astype(f32)).T.astype(bf16)
            return carry

        lax.fori_loop(0, rows, finish, 0)

    @pl.when(place == 0)
    def _():
        def finish(k, carry):
            out_buf[k] = own[k].T.astype(bf16)
            return carry

        lax.fori_loop(0, rows, finish, 0)
        drain()


def body(voltages, delays, tap_sets, tap_table, weights):
    _, channels, parts, antennas, time_len = voltages.shape
    beams = weights.shape[-1]
    set_count, tap_count = tap_table.shape
    n = lax.axis_size("station")
    tm_count = lax.axis_size("tm")
    rows = channels // n
    pad = MAXD + tap_count
    rows_in = parts * antennas
    fold_rows = rows_in * pad // time_len
    group = max(rows // 2, 1)
    sizes = (channels, parts, antennas, beams, time_len, pad, group)
    bf16, f32 = jnp.bfloat16, jnp.float32
    dma = pltpu.SemaphoreType.DMA
    in_hbm = pl.BlockSpec(memory_space=pltpu.HBM)
    operands = (
        tap_sets,
        delays,
        tap_table,
        voltages.reshape(channels, rows_in, time_len),
        weights.reshape(channels, rows_in, beams),
    )
    result = pl.pallas_call(
        functools.partial(kernel, n, tm_count, sizes),
        out_shape=pltpu.VMEM((rows, 2 * beams, time_len), bf16),
        in_specs=[in_hbm] * 5,
        out_specs=pl.BlockSpec(memory_space=pltpu.VMEM),
        scratch_shapes=[
            pltpu.SMEM(tap_sets.shape, jnp.int32),
            pltpu.SMEM(delays.shape, jnp.int32),
            pltpu.VMEM((set_count, tap_count), bf16),
            pltpu.VMEM((set_count, 1, tap_count * 128), f32),
            pltpu.VMEM((time_len, time_len), jnp.int32),
            pltpu.VMEM((pad, time_len), jnp.int32),
            pltpu.VMEM((channels, rows_in, time_len), bf16),
            pltpu.VMEM((channels, rows_in, beams), bf16),
            pltpu.VMEM((channels, fold_rows, time_len), bf16),
            pltpu.VMEM((channels, fold_rows, time_len), bf16),
            pltpu.VMEM((channels, time_len, 2 * beams), bf16),
            pltpu.VMEM((channels + rows, time_len, 2 * beams), bf16),
            pltpu.VMEM((rows, time_len, 2 * beams), f32),
            dma((3,)),
            dma((6,)),
            dma(()),
            dma((channels // group,)),
            dma(()),
            dma(((channels + rows) // group + max(group // 2, 1),)),
        ],
        compiler_params=pltpu.CompilerParams(
            collective_id=0, has_side_effects=True, vmem_limit_bytes=40 * 1024 * 1024
        ),
    )(*(x if x.ndim == 1 else pltpu.with_memory_space_constraint(x, pltpu.HBM) for x in operands))
    return result.reshape(rows, 2, beams, time_len)


def solution(mesh):
    return jax.shard_map(
        body,
        mesh=mesh,
        in_specs=(
            P(("group", "station"), "chan", None, None, "tm"),
            P(("group", "station")),
            P(("group", "station"), "chan"),
            P(),
            P(("group", "station"), "chan", None, None, None),
        ),
        out_specs=P(("group", "chan", "station"), None, None, "tm"),
        check_vma=False,
    )
```

```python
import functools

import jax
import jax.numpy as jnp
from jax import lax
from jax.experimental import pallas as pl
from jax.experimental.pallas import tpu as pltpu
from jax.sharding import PartitionSpec as P

MAXD = 16
MESH = pl.DeviceIdType.MESH
GROUPS_AHEAD = 1
LAG = 16


def kernel(
    n, tm_count, sizes, sets_hbm, delays_hbm, taps_hbm, v_hbm, w_hbm, out_buf,
    sets, delays, taps, spread, own_lag, rim_lag, v_buf, w_buf, halo_out, halo_in,
    acc_out, acc_in, own,
    small_sem, load_sem, hs_sem, hr_sem, as_sem, ar_sem,
):
    channels, parts, antennas, beams, time_len, pad, group = sizes
    rows = channels // n
    rows_in = parts * antennas
    folds = time_len // pad
    fold_rows = rows_in // folds
    set_count, tap_count = taps.shape
    head = group if n > 2 else 0
    tail = max(group // 2, 1)
    lead = GROUPS_AHEAD * group
    bf16, f32 = jnp.bfloat16, jnp.float32

    me = lax.axis_index("station")
    tm = lax.axis_index("tm")
    later, earlier = lax.rem(tm + 1, tm_count), lax.rem(tm + tm_count - 1, tm_count)

    flip = jnp.where(me >= n // 2, 1, 0)
    place = me + flip * (n - 1 - 2 * me)
    ahead_dir, back_dir = flip, 1 - flip
    ahead_count = (n - 1 - place) * rows
    back_count = (place + 1) * rows
    offset = LAG + ahead_count - back_count
    start = jnp.where(place == 0, head, 0)
    single_from = jnp.where(place < n // 2 - 1, ahead_count - tail, ahead_count)
    shared = (channels + rows) // group

    def channel_of(station, k):
        return (station + flip * (n - 1 - 2 * station)) * rows + k

    def ahead_channel(i):
        return channel_of(n - 1 - i // rows, lax.rem(i, rows))

    def back_channel(j):
        return channel_of(j // rows, lax.rem(j, rows))

    def load(first, count, sems):
        span = pl.ds(first, count)
        return (
            pltpu.make_async_copy(v_hbm.at[span], v_buf.at[span], load_sem.at[sems]),
            pltpu.make_async_copy(w_hbm.at[span], w_buf.at[span], load_sem.at[sems + 1]),
        )

    def halo_copy(ch):
        span = pl.ds(ch, group)
        return pltpu.make_async_remote_copy(
            src_ref=halo_out.at[span],
            dst_ref=halo_in.at[span],
            send_sem=hs_sem,
            recv_sem=hr_sem.at[ch // group],
            device_id={"tm": later},
            device_id_type=MESH,
        )

    def sum_copy(ch, direction, single=False):
        target = me + 1 - 2 * direction
        final = (ch // rows == target) & (direction == 1)
        slot = jnp.where(final, channels + lax.rem(ch, rows), ch)
        return pltpu.make_async_remote_copy(
            src_ref=acc_out.at[ch],
            dst_ref=acc_in.at[slot],
            send_sem=as_sem,
            recv_sem=ar_sem.at[jnp.where(single, shared + lax.rem(ch, tail), slot // group)],
            device_id={"station": target},
            device_id_type=MESH,
        )

    def arrival(ch, direction):
        final = (ch // rows == me) & (direction == 1)
        return jnp.where(final, channels + lax.rem(ch, rows), ch)

    def wait_group(slot, count=group):
        span = acc_in.at[pl.ds(slot, count)]
        pltpu.make_async_copy(span, span, ar_sem.at[slot // group]).wait()

    def wait_single(slot):
        sem = ar_sem.at[shared + lax.rem(slot, tail)]
        pltpu.make_async_copy(acc_in.at[slot], acc_in.at[slot], sem).wait()

    late_rows, early_rows = pl.ds(pad, time_len - pad), pl.ds(0, pad)

    def piece_copy(i, piece, count=1):
        ch = ahead_channel(i)
        span = pl.ds(ch, count)
        return pltpu.make_async_remote_copy(
            src_ref=acc_out.at[span, piece],
            dst_ref=acc_in.at[span, piece],
            send_sem=as_sem,
            recv_sem=ar_sem.at[ch // group],
            device_id={"station": me + 1 - 2 * ahead_dir},
            device_id_type=MESH,
        )

    small = [
        pltpu.make_async_copy(taps_hbm, taps, small_sem.at[0]),
        pltpu.make_async_copy(delays_hbm, delays, small_sem.at[1]),
        pltpu.make_async_copy(sets_hbm, sets, small_sem.at[2]),
    ]
    first = ahead_channel(0)
    first_loads, head_loads = load(first, 1, 0), load(first + 1, group - 1, 4)
    for copy in first_loads + head_loads:
        copy.start()
    for copy in small:
        copy.start()

    barrier = pltpu.get_barrier_semaphore()

    @pl.when(me > 0)
    def _():
        pl.semaphore_signal(barrier, inc=1, device_id={"station": me - 1}, device_id_type=MESH)

    @pl.when(me < n - 1)
    def _():
        pl.semaphore_signal(barrier, inc=1, device_id={"station": me + 1}, device_id_type=MESH)

    for target in ({"tm": earlier}, {"tm": later}):
        pl.semaphore_signal(barrier, inc=1, device_id=target, device_id_type=MESH)

    for copy in load(first + max(head, group), rows - max(head, group), 2):
        copy.start()

    def load_rest(station, carry):
        for copy in load(channel_of(station, 0), rows, 2):
            copy.start()
        return carry

    lax.fori_loop(0, n - 1, load_rest, 0)

    from_row = lax.broadcasted_iota(jnp.int32, (folds * time_len, time_len), 0)
    to_lane = lax.broadcasted_iota(jnp.int32, (folds * time_len, time_len), 1)
    wanted = (to_lane // pad) * time_len + lax.rem(to_lane, pad) + time_len - pad
    picker = (from_row == wanted).astype(f32).astype(bf16)

    for copy in small:
        copy.wait()

    pick_tap = lax.broadcasted_iota(jnp.int32, (tap_count, tap_count * 128), 1) // 128
    tap_row = lax.broadcasted_iota(jnp.int32, (tap_count, tap_count * 128), 0)
    chosen = (pick_tap == tap_row).astype(f32).astype(bf16)
    values = jnp.dot(taps[...], chosen, preferred_element_type=f32)
    for m in range(set_count):
        spread[m] = values[m:m + 1]

    out_pos = lax.broadcasted_iota(jnp.int32, (time_len, time_len), 0)
    in_pos = lax.broadcasted_iota(jnp.int32, (time_len, time_len), 1)
    own_lag[...] = out_pos - in_pos - delays[0]
    rim_out = lax.broadcasted_iota(jnp.int32, (pad, time_len), 0)
    rim_in = lax.rem(lax.broadcasted_iota(jnp.int32, (pad, time_len), 1), pad) - pad
    rim_lag[...] = jnp.where(tm > 0, rim_out - rim_in - delays[0], -1)

    fold_lane = lax.broadcasted_iota(jnp.int32, (fold_rows, time_len), 1) // pad

    def toeplitz(m, lag):
        values = jnp.zeros(lag.shape, f32)
        for k in range(tap_count):
            values = jnp.where(lag == k, spread[m, :, pl.ds(k * 128, 128)], values)
        return values.astype(bf16)

    def rims_of(ch):
        rim = halo_in[ch]
        return jnp.concatenate(
            [jnp.where(fold_lane == q, rim, jnp.zeros_like(rim)) for q in range(folds)], axis=0
        )

    def filtered(filt, window):
        return lax.dot_general(
            filt, window, (((1,), (1,)), ((), ())), preferred_element_type=f32
        ).astype(bf16)

    def steered(ch, delayed):
        wr = w_buf[ch, pl.ds(0, antennas), :]
        wi = w_buf[ch, pl.ds(antennas, antennas), :]
        steer = jnp.concatenate(
            [jnp.concatenate([wr, wi], axis=1), jnp.concatenate([-wi, wr], axis=1)], axis=0
        )
        return jnp.dot(delayed, steer, preferred_element_type=f32)

    def beams_of(ch):
        @pl.when(lax.rem(ch, group) == 0)
        def _():
            halo_copy(ch).wait_recv()

        m = sets[0, ch]
        rim = toeplitz(m, rim_lag[...])
        rim = jnp.concatenate([rim, jnp.zeros((time_len - pad, time_len), bf16)], axis=0)
        filt = jnp.concatenate([toeplitz(m, own_lag[...]), rim], axis=1)
        window = jnp.concatenate([v_buf[ch], rims_of(ch)], axis=1)
        return steered(ch, filtered(filt, window))

    def pack(ch):
        span = pl.ds(ch, group)
        wide = jnp.concatenate(
            [
                v_buf[span, pl.ds(q * fold_rows, fold_rows), :].reshape(group * fold_rows, time_len)
                for q in range(folds)
            ],
            axis=1,
        )
        packed = jnp.dot(wide, picker, preferred_element_type=f32).astype(bf16)
        halo_out[span] = packed.reshape(group, fold_rows, time_len)
        halo_copy(ch).start()

    def late_rows_of(i):
        ch = ahead_channel(i)
        filt = toeplitz(sets[0, ch], own_lag[late_rows, :])
        total = steered(ch, filtered(filt, v_buf[ch]))
        acc_out[ch, late_rows, :] = total.astype(bf16)

    for copy in first_loads:
        copy.wait()

    if head:
        @pl.when(place == 0)
        def _():
            late_rows_of(0)

    present = 2 + jnp.where(me > 0, 1, 0) + jnp.where(me < n - 1, 1, 0)
    pl.semaphore_wait(barrier, present)

    def send_late(i, carry):
        late_rows_of(i)
        piece_copy(i, late_rows).start()
        return carry

    cut = jnp.where(lax.axis_index("chan") > 0, min(3, head), head)

    if head:
        @pl.when(place == 0)
        def _():
            piece_copy(0, late_rows).start()

            for copy in head_loads:
                copy.wait()

            lax.fori_loop(1, cut, send_late, 0)

            pack(first)

    @pl.when(place > 0)
    def _():
        for copy in head_loads:
            copy.wait()

    for copy in load(0, channels - max(head, group), 2):
        copy.wait()

    def pack_first(g, carry):
        pack(ahead_channel(start + g * group))
        return carry

    lax.fori_loop(0, lead // group, pack_first, 0)


    if head:
        @pl.when(place == 0)
        def _():
            def send_early(i, carry):
                ch = ahead_channel(i)
                m = sets[0, ch]
                filt = jnp.concatenate(
                    [toeplitz(m, own_lag[early_rows, :]), toeplitz(m, rim_lag[...])], axis=1
                )
                window = jnp.concatenate([v_buf[ch], rims_of(ch)], axis=1)
                total = steered(ch, filtered(filt, window))
                acc_out[ch, early_rows, :] = total.astype(bf16)
                return carry

            halo_copy(first).wait_recv()
            lax.fori_loop(cut, head, send_late, 0)
            lax.fori_loop(0, head, send_early, 0)
            piece_copy(0, early_rows, head).start()

    def step(i, carry):
        j = i - offset

        @pl.when((i + lead < ahead_count) & (lax.rem(i, group) == 0))
        def _():
            pack(ahead_channel(i + lead))

        @pl.when((j + lead >= 0) & (j + lead < back_count) & (lax.rem(j + lead, group) == 0))
        def _():
            pack(back_channel(j + lead))

        @pl.when(i < ahead_count)
        def _():
            ch = ahead_channel(i)
            total = beams_of(ch)

            @pl.when(place > 0)
            def _():
                @pl.when(lax.rem(i, group) == 0)
                def _():
                    wait_group(ch)

                acc_out[ch] = (total + acc_in[ch].astype(f32)).astype(bf16)

            @pl.when(place == 0)
            def _():
                acc_out[ch] = total.astype(bf16)

            sum_copy(ch, ahead_dir, i >= single_from).start()

        @pl.when((j >= 0) & (j < back_count))
        def _():
            ch = back_channel(j)
            total = beams_of(ch)
            slot = arrival(ch, back_dir)

            @pl.when(lax.rem(j, group) == 0)
            def _():
                wait_group(slot)

            total = total + acc_in[slot].astype(f32)

            @pl.when(j < place * rows)
            def _():
                acc_out[ch] = total.astype(bf16)
                sum_copy(ch, back_dir).start()

            @pl.when(j >= place * rows)
            def _():
                own[lax.rem(j, rows)] = total

        return carry

    lax.fori_loop(start, ahead_count + LAG, step, 0)

    def drain():
        pltpu.make_async_remote_copy(
            src_ref=halo_out,
            dst_ref=halo_in,
            send_sem=hs_sem,
            recv_sem=hr_sem.at[0],
            device_id={"tm": later},
            device_id_type=MESH,
        ).wait_send()
        sent = pl.ds(0, (n - 1) * rows)
        pltpu.make_async_remote_copy(
            src_ref=acc_out.at[sent],
            dst_ref=acc_in.at[sent],
            send_sem=as_sem,
            recv_sem=ar_sem.at[0],
            device_id={"tm": later},
            device_id_type=MESH,
        ).wait_send()

    @pl.when(place > 0)
    def _():
        drain()

        def finish(k, carry):
            slot = arrival(me * rows + k, ahead_dir)
            @pl.when(k >= rows - tail)
            def _():
                wait_single(slot)

            @pl.when((k < rows - group) & (lax.rem(k, group) == 0))
            def _():
                wait_group(slot)

            if group > tail:
                @pl.when(k == rows - group)
                def _():
                    wait_group(slot, group - tail)

            out_buf[k] = (own[k] + acc_in[slot].astype(f32)).T.astype(bf16)
            return carry

        lax.fori_loop(0, rows, finish, 0)

    @pl.when(place == 0)
    def _():
        def finish(k, carry):
            out_buf[k] = own[k].T.astype(bf16)
            return carry

        lax.fori_loop(0, rows, finish, 0)
        drain()


def body(voltages, delays, tap_sets, tap_table, weights):
    _, channels, parts, antennas, time_len = voltages.shape
    beams = weights.shape[-1]
    set_count, tap_count = tap_table.shape
    n = lax.axis_size("station")
    tm_count = lax.axis_size("tm")
    rows = channels // n
    pad = MAXD + tap_count
    rows_in = parts * antennas
    fold_rows = rows_in * pad // time_len
    group = max(rows // 2, 1)
    sizes = (channels, parts, antennas, beams, time_len, pad, group)
    bf16, f32 = jnp.bfloat16, jnp.float32
    dma = pltpu.SemaphoreType.DMA
    in_hbm = pl.BlockSpec(memory_space=pltpu.HBM)
    operands = (
        tap_sets,
        delays,
        tap_table,
        voltages.reshape(channels, rows_in, time_len),
        weights.reshape(channels, rows_in, beams),
    )
    result = pl.pallas_call(
        functools.partial(kernel, n, tm_count, sizes),
        out_shape=pltpu.VMEM((rows, 2 * beams, time_len), bf16),
        in_specs=[in_hbm] * 5,
        out_specs=pl.BlockSpec(memory_space=pltpu.VMEM),
        scratch_shapes=[
            pltpu.SMEM(tap_sets.shape, jnp.int32),
            pltpu.SMEM(delays.shape, jnp.int32),
            pltpu.VMEM((set_count, tap_count), bf16),
            pltpu.VMEM((set_count, 1, tap_count * 128), f32),
            pltpu.VMEM((time_len, time_len), jnp.int32),
            pltpu.VMEM((pad, time_len), jnp.int32),
            pltpu.VMEM((channels, rows_in, time_len), bf16),
            pltpu.VMEM((channels, rows_in, beams), bf16),
            pltpu.VMEM((channels, fold_rows, time_len), bf16),
            pltpu.VMEM((channels, fold_rows, time_len), bf16),
            pltpu.VMEM((channels, time_len, 2 * beams), bf16),
            pltpu.VMEM((channels + rows, time_len, 2 * beams), bf16),
            pltpu.VMEM((rows, time_len, 2 * beams), f32),
            dma((3,)),
            dma((6,)),
            dma(()),
            dma((channels // group,)),
            dma(()),
            dma(((channels + rows) // group + max(group // 2, 1),)),
        ],
        compiler_params=pltpu.CompilerParams(
            collective_id=0, has_side_effects=True, vmem_limit_bytes=40 * 1024 * 1024
        ),
    )(*(x if x.ndim == 1 else pltpu.with_memory_space_constraint(x, pltpu.HBM) for x in operands))
    return result.reshape(rows, 2, beams, time_len)


def solution(mesh):
    return jax.shard_map(
        body,
        mesh=mesh,
        in_specs=(
            P(("group", "station"), "chan", None, None, "tm"),
            P(("group", "station")),
            P(("group", "station"), "chan"),
            P(),
            P(("group", "station"), "chan", None, None, None),
        ),
        out_specs=P(("group", "chan", "station"), None, None, "tm"),
        check_vma=False,
    )
```

```python
import functools

import jax
import jax.numpy as jnp
from jax import lax
from jax.experimental import pallas as pl
from jax.experimental.pallas import tpu as pltpu
from jax.sharding import PartitionSpec as P

MAXD = 16
MESH = pl.DeviceIdType.MESH
GROUPS_AHEAD = 1
LAG = 16


def kernel(
    n, tm_count, sizes, sets_hbm, delays_hbm, taps_hbm, v_hbm, w_hbm, out_buf,
    sets, delays, taps, spread, own_lag, rim_lag, v_buf, w_buf, halo_out, halo_in,
    acc_out, acc_in, own,
    small_sem, load_sem, hs_sem, hr_sem, as_sem, ar_sem,
):
    channels, parts, antennas, beams, time_len, pad, group = sizes
    rows = channels // n
    rows_in = parts * antennas
    folds = time_len // pad
    fold_rows = rows_in // folds
    set_count, tap_count = taps.shape
    head = group if n > 2 else 0
    tail = max(group // 2, 1)
    lead = GROUPS_AHEAD * group
    bf16, f32 = jnp.bfloat16, jnp.float32

    me = lax.axis_index("station")
    tm = lax.axis_index("tm")
    later, earlier = lax.rem(tm + 1, tm_count), lax.rem(tm + tm_count - 1, tm_count)

    flip = jnp.where(me >= n // 2, 1, 0)
    place = me + flip * (n - 1 - 2 * me)
    ahead_dir, back_dir = flip, 1 - flip
    ahead_count = (n - 1 - place) * rows
    back_count = (place + 1) * rows
    offset = LAG + ahead_count - back_count
    start = jnp.where(place == 0, head, 0)
    single_from = jnp.where(place < n // 2 - 1, ahead_count - tail, ahead_count)
    shared = (channels + rows) // group

    def channel_of(station, k):
        return (station + flip * (n - 1 - 2 * station)) * rows + k

    def ahead_channel(i):
        return channel_of(n - 1 - i // rows, lax.rem(i, rows))

    def back_channel(j):
        return channel_of(j // rows, lax.rem(j, rows))

    def load(first, count, sems):
        span = pl.ds(first, count)
        return (
            pltpu.make_async_copy(v_hbm.at[span], v_buf.at[span], load_sem.at[sems]),
            pltpu.make_async_copy(w_hbm.at[span], w_buf.at[span], load_sem.at[sems + 1]),
        )

    def halo_copy(ch):
        span = pl.ds(ch, group)
        return pltpu.make_async_remote_copy(
            src_ref=halo_out.at[span],
            dst_ref=halo_in.at[span],
            send_sem=hs_sem,
            recv_sem=hr_sem.at[ch // group],
            device_id={"tm": later},
            device_id_type=MESH,
        )

    def sum_copy(ch, direction, single=False):
        target = me + 1 - 2 * direction
        final = (ch // rows == target) & (direction == 1)
        slot = jnp.where(final, channels + lax.rem(ch, rows), ch)
        return pltpu.make_async_remote_copy(
            src_ref=acc_out.at[ch],
            dst_ref=acc_in.at[slot],
            send_sem=as_sem,
            recv_sem=ar_sem.at[jnp.where(single, shared + lax.rem(ch, tail), slot // group)],
            device_id={"station": target},
            device_id_type=MESH,
        )

    def arrival(ch, direction):
        final = (ch // rows == me) & (direction == 1)
        return jnp.where(final, channels + lax.rem(ch, rows), ch)

    def wait_group(slot, count=group):
        span = acc_in.at[pl.ds(slot, count)]
        pltpu.make_async_copy(span, span, ar_sem.at[slot // group]).wait()

    def wait_single(slot):
        sem = ar_sem.at[shared + lax.rem(slot, tail)]
        pltpu.make_async_copy(acc_in.at[slot], acc_in.at[slot], sem).wait()

    late_rows, early_rows = pl.ds(pad, time_len - pad), pl.ds(0, pad)

    def piece_copy(i, piece):
        ch = ahead_channel(i)
        return pltpu.make_async_remote_copy(
            src_ref=acc_out.at[ch, piece],
            dst_ref=acc_in.at[ch, piece],
            send_sem=as_sem,
            recv_sem=ar_sem.at[ch // group],
            device_id={"station": me + 1 - 2 * ahead_dir},
            device_id_type=MESH,
        )

    small = [
        pltpu.make_async_copy(taps_hbm, taps, small_sem.at[0]),
        pltpu.make_async_copy(delays_hbm, delays, small_sem.at[1]),
        pltpu.make_async_copy(sets_hbm, sets, small_sem.at[2]),
    ]
    first = ahead_channel(0)
    first_loads, head_loads = load(first, 1, 0), load(first + 1, group - 1, 4)
    for copy in first_loads + head_loads:
        copy.start()
    for copy in small:
        copy.start()

    barrier = pltpu.get_barrier_semaphore()

    @pl.when(me > 0)
    def _():
        pl.semaphore_signal(barrier, inc=1, device_id={"station": me - 1}, device_id_type=MESH)

    @pl.when(me < n - 1)
    def _():
        pl.semaphore_signal(barrier, inc=1, device_id={"station": me + 1}, device_id_type=MESH)

    sides = (earlier, later) if tm_count > 2 else (later,)
    for side in sides:
        pl.semaphore_signal(barrier, inc=1, device_id={"tm": side}, device_id_type=MESH)

    for copy in load(first + max(head, group), rows - max(head, group), 2):
        copy.start()

    def load_rest(station, carry):
        for copy in load(channel_of(station, 0), rows, 2):
            copy.start()
        return carry

    lax.fori_loop(0, n - 1, load_rest, 0)

    from_row = lax.broadcasted_iota(jnp.int32, (folds * time_len, time_len), 0)
    to_lane = lax.broadcasted_iota(jnp.int32, (folds * time_len, time_len), 1)
    wanted = (to_lane // pad) * time_len + lax.rem(to_lane, pad) + time_len - pad
    picker = (from_row == wanted).astype(f32).astype(bf16)

    for copy in small:
        copy.wait()

    pick_tap = lax.broadcasted_iota(jnp.int32, (tap_count, tap_count * 128), 1) // 128
    tap_row = lax.broadcasted_iota(jnp.int32, (tap_count, tap_count * 128), 0)
    chosen = (pick_tap == tap_row).astype(f32).astype(bf16)
    values = jnp.dot(taps[...], chosen, preferred_element_type=f32)
    for m in range(set_count):
        spread[m] = values[m:m + 1]

    out_pos = lax.broadcasted_iota(jnp.int32, (time_len, time_len), 0)
    in_pos = lax.broadcasted_iota(jnp.int32, (time_len, time_len), 1)
    own_lag[...] = out_pos - in_pos - delays[0]
    rim_out = lax.broadcasted_iota(jnp.int32, (pad, time_len), 0)
    rim_in = lax.rem(lax.broadcasted_iota(jnp.int32, (pad, time_len), 1), pad) - pad
    rim_lag[...] = jnp.where(tm > 0, rim_out - rim_in - delays[0], -1)

    fold_lane = lax.broadcasted_iota(jnp.int32, (fold_rows, time_len), 1) // pad

    def toeplitz(m, lag):
        values = jnp.zeros(lag.shape, f32)
        for k in range(tap_count):
            values = jnp.where(lag == k, spread[m, :, pl.ds(k * 128, 128)], values)
        return values.astype(bf16)

    def rims_of(ch):
        rim = halo_in[ch]
        return jnp.concatenate(
            [jnp.where(fold_lane == q, rim, jnp.zeros_like(rim)) for q in range(folds)], axis=0
        )

    def filtered(filt, window):
        return lax.dot_general(
            filt, window, (((1,), (1,)), ((), ())), preferred_element_type=f32
        ).astype(bf16)

    def steered(ch, delayed):
        wr = w_buf[ch, pl.ds(0, antennas), :]
        wi = w_buf[ch, pl.ds(antennas, antennas), :]
        steer = jnp.concatenate(
            [jnp.concatenate([wr, wi], axis=1), jnp.concatenate([-wi, wr], axis=1)], axis=0
        )
        return jnp.dot(delayed, steer, preferred_element_type=f32)

    def beams_of(ch):
        @pl.when(lax.rem(ch, group) == 0)
        def _():
            halo_copy(ch).wait_recv()

        m = sets[0, ch]
        rim = toeplitz(m, rim_lag[...])
        rim = jnp.concatenate([rim, jnp.zeros((time_len - pad, time_len), bf16)], axis=0)
        filt = jnp.concatenate([toeplitz(m, own_lag[...]), rim], axis=1)
        window = jnp.concatenate([v_buf[ch], rims_of(ch)], axis=1)
        return steered(ch, filtered(filt, window))

    def pack(ch):
        span = pl.ds(ch, group)
        wide = jnp.concatenate(
            [
                v_buf[span, pl.ds(q * fold_rows, fold_rows), :].reshape(group * fold_rows, time_len)
                for q in range(folds)
            ],
            axis=1,
        )
        packed = jnp.dot(wide, picker, preferred_element_type=f32).astype(bf16)
        halo_out[span] = packed.reshape(group, fold_rows, time_len)
        halo_copy(ch).start()

    def late_rows_of(i):
        ch = ahead_channel(i)
        filt = toeplitz(sets[0, ch], own_lag[late_rows, :])
        total = steered(ch, filtered(filt, v_buf[ch]))
        acc_out[ch, late_rows, :] = total.astype(bf16)

    for copy in first_loads:
        copy.wait()

    if head:
        @pl.when(place == 0)
        def _():
            late_rows_of(0)

    present = len(sides) + jnp.where(me > 0, 1, 0) + jnp.where(me < n - 1, 1, 0)
    pl.semaphore_wait(barrier, present)

    def send_late(i, carry):
        late_rows_of(i)
        piece_copy(i, late_rows).start()
        return carry

    if head:
        @pl.when(place == 0)
        def _():
            piece_copy(0, late_rows).start()

            for copy in head_loads:
                copy.wait()

            lax.fori_loop(1, head, send_late, 0)

            pack(first)

    @pl.when(place > 0)
    def _():
        for copy in head_loads:
            copy.wait()

    for copy in load(0, channels - max(head, group), 2):
        copy.wait()

    def pack_first(g, carry):
        pack(ahead_channel(start + g * group))
        return carry

    lax.fori_loop(0, lead // group, pack_first, 0)

    if head:
        @pl.when(place == 0)
        def _():
            def send_early(i, carry):
                ch = ahead_channel(i)

                @pl.when(lax.rem(i, group) == 0)
                def _():
                    halo_copy(ch).wait_recv()

                m = sets[0, ch]
                filt = jnp.concatenate(
                    [toeplitz(m, own_lag[early_rows, :]), toeplitz(m, rim_lag[...])], axis=1
                )
                window = jnp.concatenate([v_buf[ch], rims_of(ch)], axis=1)
                total = steered(ch, filtered(filt, window))
                acc_out[ch, early_rows, :] = total.astype(bf16)
                piece_copy(i, early_rows).start()
                return carry

            lax.fori_loop(0, head, send_early, 0)

    def step(i, carry):
        j = i - offset

        @pl.when((i + lead < ahead_count) & (lax.rem(i, group) == 0))
        def _():
            pack(ahead_channel(i + lead))

        @pl.when((j + lead >= 0) & (j + lead < back_count) & (lax.rem(j + lead, group) == 0))
        def _():
            pack(back_channel(j + lead))

        @pl.when(i < ahead_count)
        def _():
            ch = ahead_channel(i)
            total = beams_of(ch)

            @pl.when(place > 0)
            def _():
                @pl.when(lax.rem(i, group) == 0)
                def _():
                    wait_group(ch)

                acc_out[ch] = (total + acc_in[ch].astype(f32)).astype(bf16)

            @pl.when(place == 0)
            def _():
                acc_out[ch] = total.astype(bf16)

            sum_copy(ch, ahead_dir, i >= single_from).start()

        @pl.when((j >= 0) & (j < back_count))
        def _():
            ch = back_channel(j)
            total = beams_of(ch)
            slot = arrival(ch, back_dir)

            @pl.when(lax.rem(j, group) == 0)
            def _():
                wait_group(slot)

            total = total + acc_in[slot].astype(f32)

            @pl.when(j < place * rows)
            def _():
                acc_out[ch] = total.astype(bf16)
                sum_copy(ch, back_dir).start()

            @pl.when(j >= place * rows)
            def _():
                own[lax.rem(j, rows)] = total

        return carry

    lax.fori_loop(start, ahead_count + LAG, step, 0)

    def drain():
        pltpu.make_async_remote_copy(
            src_ref=halo_out,
            dst_ref=halo_in,
            send_sem=hs_sem,
            recv_sem=hr_sem.at[0],
            device_id={"tm": later},
            device_id_type=MESH,
        ).wait_send()
        sent = pl.ds(0, (n - 1) * rows)
        pltpu.make_async_remote_copy(
            src_ref=acc_out.at[sent],
            dst_ref=acc_in.at[sent],
            send_sem=as_sem,
            recv_sem=ar_sem.at[0],
            device_id={"tm": later},
            device_id_type=MESH,
        ).wait_send()

    @pl.when(place > 0)
    def _():
        drain()

        def finish(k, carry):
            slot = arrival(me * rows + k, ahead_dir)
            @pl.when(k >= rows - tail)
            def _():
                wait_single(slot)

            @pl.when((k < rows - group) & (lax.rem(k, group) == 0))
            def _():
                wait_group(slot)

            if group > tail:
                @pl.when(k == rows - group)
                def _():
                    wait_group(slot, group - tail)

            out_buf[k] = (own[k] + acc_in[slot].astype(f32)).T.astype(bf16)
            return carry

        lax.fori_loop(0, rows, finish, 0)

    @pl.when(place == 0)
    def _():
        def finish(k, carry):
            out_buf[k] = own[k].T.astype(bf16)
            return carry

        lax.fori_loop(0, rows, finish, 0)
        drain()


def body(voltages, delays, tap_sets, tap_table, weights):
    _, channels, parts, antennas, time_len = voltages.shape
    beams = weights.shape[-1]
    set_count, tap_count = tap_table.shape
    n = lax.axis_size("station")
    tm_count = lax.axis_size("tm")
    rows = channels // n
    pad = MAXD + tap_count
    rows_in = parts * antennas
    fold_rows = rows_in * pad // time_len
    group = max(rows // 2, 1)
    sizes = (channels, parts, antennas, beams, time_len, pad, group)
    bf16, f32 = jnp.bfloat16, jnp.float32
    dma = pltpu.SemaphoreType.DMA
    in_hbm = pl.BlockSpec(memory_space=pltpu.HBM)
    operands = (
        tap_sets,
        delays,
        tap_table,
        voltages.reshape(channels, rows_in, time_len),
        weights.reshape(channels, rows_in, beams),
    )
    result = pl.pallas_call(
        functools.partial(kernel, n, tm_count, sizes),
        out_shape=pltpu.VMEM((rows, 2 * beams, time_len), bf16),
        in_specs=[in_hbm] * 5,
        out_specs=pl.BlockSpec(memory_space=pltpu.VMEM),
        scratch_shapes=[
            pltpu.SMEM(tap_sets.shape, jnp.int32),
            pltpu.SMEM(delays.shape, jnp.int32),
            pltpu.VMEM((set_count, tap_count), bf16),
            pltpu.VMEM((set_count, 1, tap_count * 128), f32),
            pltpu.VMEM((time_len, time_len), jnp.int32),
            pltpu.VMEM((pad, time_len), jnp.int32),
            pltpu.VMEM((channels, rows_in, time_len), bf16),
            pltpu.VMEM((channels, rows_in, beams), bf16),
            pltpu.VMEM((channels, fold_rows, time_len), bf16),
            pltpu.VMEM((channels, fold_rows, time_len), bf16),
            pltpu.VMEM((channels, time_len, 2 * beams), bf16),
            pltpu.VMEM((channels + rows, time_len, 2 * beams), bf16),
            pltpu.VMEM((rows, time_len, 2 * beams), f32),
            dma((3,)),
            dma((6,)),
            dma(()),
            dma((channels // group,)),
            dma(()),
            dma(((channels + rows) // group + max(group // 2, 1),)),
        ],
        compiler_params=pltpu.CompilerParams(
            collective_id=0, has_side_effects=True, vmem_limit_bytes=40 * 1024 * 1024
        ),
    )(*(x if x.ndim == 1 else pltpu.with_memory_space_constraint(x, pltpu.HBM) for x in operands))
    return result.reshape(rows, 2, beams, time_len)


def solution(mesh):
    return jax.shard_map(
        body,
        mesh=mesh,
        in_specs=(
            P(("group", "station"), "chan", None, None, "tm"),
            P(("group", "station")),
            P(("group", "station"), "chan"),
            P(),
            P(("group", "station"), "chan", None, None, None),
        ),
        out_specs=P(("group", "chan", "station"), None, None, "tm"),
        check_vma=False,
    )
```

```python
import functools

import jax
import jax.numpy as jnp
from jax import lax
from jax.experimental import pallas as pl
from jax.experimental.pallas import tpu as pltpu
from jax.sharding import PartitionSpec as P

MAXD = 16
MESH = pl.DeviceIdType.MESH
GROUPS_AHEAD = 1
LAG = 16


def kernel(
    n, tm_count, sizes, sets_hbm, delays_hbm, taps_hbm, v_hbm, w_hbm, out_buf,
    sets, delays, taps, spread, own_lag, rim_lag, v_buf, w_buf, halo_out, halo_in,
    acc_out, acc_in, own,
    small_sem, load_sem, hs_sem, hr_sem, as_sem, ar_sem,
):
    channels, parts, antennas, beams, time_len, pad, group = sizes
    rows = channels // n
    rows_in = parts * antennas
    folds = time_len // pad
    fold_rows = rows_in // folds
    set_count, tap_count = taps.shape
    head = group if n > 2 else 0
    tail = max(group // 2, 1)
    lead = GROUPS_AHEAD * group
    bf16, f32 = jnp.bfloat16, jnp.float32

    me = lax.axis_index("station")
    tm = lax.axis_index("tm")
    later, earlier = lax.rem(tm + 1, tm_count), lax.rem(tm + tm_count - 1, tm_count)

    flip = jnp.where(me >= n // 2, 1, 0)
    place = me + flip * (n - 1 - 2 * me)
    ahead_dir, back_dir = flip, 1 - flip
    ahead_count = (n - 1 - place) * rows
    back_count = (place + 1) * rows
    offset = LAG + ahead_count - back_count
    start = jnp.where(place == 0, head, 0)
    single_from = jnp.where(place < n // 2 - 1, ahead_count - tail, ahead_count)
    shared = (channels + rows) // group

    def channel_of(station, k):
        return (station + flip * (n - 1 - 2 * station)) * rows + k

    def ahead_channel(i):
        return channel_of(n - 1 - i // rows, lax.rem(i, rows))

    def back_channel(j):
        return channel_of(j // rows, lax.rem(j, rows))

    def load(first, count, sems):
        span = pl.ds(first, count)
        return (
            pltpu.make_async_copy(v_hbm.at[span], v_buf.at[span], load_sem.at[sems]),
            pltpu.make_async_copy(w_hbm.at[span], w_buf.at[span], load_sem.at[sems + 1]),
        )

    def halo_copy(ch):
        span = pl.ds(ch, group)
        return pltpu.make_async_remote_copy(
            src_ref=halo_out.at[span],
            dst_ref=halo_in.at[span],
            send_sem=hs_sem,
            recv_sem=hr_sem.at[ch // group],
            device_id={"tm": later},
            device_id_type=MESH,
        )

    def sum_copy(ch, direction, single=False):
        target = me + 1 - 2 * direction
        final = (ch // rows == target) & (direction == 1)
        slot = jnp.where(final, channels + lax.rem(ch, rows), ch)
        return pltpu.make_async_remote_copy(
            src_ref=acc_out.at[ch],
            dst_ref=acc_in.at[slot],
            send_sem=as_sem,
            recv_sem=ar_sem.at[jnp.where(single, shared + lax.rem(ch, tail), slot // group)],
            device_id={"station": target},
            device_id_type=MESH,
        )

    def arrival(ch, direction):
        final = (ch // rows == me) & (direction == 1)
        return jnp.where(final, channels + lax.rem(ch, rows), ch)

    def wait_group(slot, count=group):
        span = acc_in.at[pl.ds(slot, count)]
        pltpu.make_async_copy(span, span, ar_sem.at[slot // group]).wait()

    def wait_single(slot):
        sem = ar_sem.at[shared + lax.rem(slot, tail)]
        pltpu.make_async_copy(acc_in.at[slot], acc_in.at[slot], sem).wait()

    late_rows, early_rows = pl.ds(pad, time_len - pad), pl.ds(0, pad)

    def piece_copy(i, piece):
        ch = ahead_channel(i)
        return pltpu.make_async_remote_copy(
            src_ref=acc_out.at[ch, piece],
            dst_ref=acc_in.at[ch, piece],
            send_sem=as_sem,
            recv_sem=ar_sem.at[ch // group],
            device_id={"station": me + 1 - 2 * ahead_dir},
            device_id_type=MESH,
        )

    small = [
        pltpu.make_async_copy(taps_hbm, taps, small_sem.at[0]),
        pltpu.make_async_copy(delays_hbm, delays, small_sem.at[1]),
        pltpu.make_async_copy(sets_hbm, sets, small_sem.at[2]),
    ]
    first = ahead_channel(0)
    first_loads, head_loads = load(first, 1, 0), load(first + 1, group - 1, 4)
    for copy in first_loads + head_loads:
        copy.start()
    for copy in small:
        copy.start()

    barrier = pltpu.get_barrier_semaphore()

    @pl.when(me > 0)
    def _():
        pl.semaphore_signal(barrier, inc=1, device_id={"station": me - 1}, device_id_type=MESH)

    @pl.when(me < n - 1)
    def _():
        pl.semaphore_signal(barrier, inc=1, device_id={"station": me + 1}, device_id_type=MESH)

    sides = (earlier, later) if tm_count > 2 else (later,)
    for side in sides:
        pl.semaphore_signal(barrier, inc=1, device_id={"tm": side}, device_id_type=MESH)

    for copy in load(first + max(head, group), rows - max(head, group), 2):
        copy.start()

    def load_rest(station, carry):
        for copy in load(channel_of(station, 0), rows, 2):
            copy.start()
        return carry

    lax.fori_loop(0, n - 1, load_rest, 0)

    from_row = lax.broadcasted_iota(jnp.int32, (folds * time_len, time_len), 0)
    to_lane = lax.broadcasted_iota(jnp.int32, (folds * time_len, time_len), 1)
    wanted = (to_lane // pad) * time_len + lax.rem(to_lane, pad) + time_len - pad
    picker = (from_row == wanted).astype(f32).astype(bf16)

    for copy in small:
        copy.wait()

    pick_tap = lax.broadcasted_iota(jnp.int32, (tap_count, tap_count * 128), 1) // 128
    tap_row = lax.broadcasted_iota(jnp.int32, (tap_count, tap_count * 128), 0)
    chosen = (pick_tap == tap_row).astype(f32).astype(bf16)
    values = jnp.dot(taps[...], chosen, preferred_element_type=f32)
    for m in range(set_count):
        spread[m] = values[m:m + 1]

    out_pos = lax.broadcasted_iota(jnp.int32, (time_len, time_len), 0)
    in_pos = lax.broadcasted_iota(jnp.int32, (time_len, time_len), 1)
    own_lag[...] = out_pos - in_pos - delays[0]
    rim_out = lax.broadcasted_iota(jnp.int32, (pad, time_len), 0)
    rim_in = lax.rem(lax.broadcasted_iota(jnp.int32, (pad, time_len), 1), pad) - pad
    rim_lag[...] = jnp.where(tm > 0, rim_out - rim_in - delays[0], -1)

    fold_lane = lax.broadcasted_iota(jnp.int32, (fold_rows, time_len), 1) // pad

    def toeplitz(m, lag):
        values = jnp.zeros(lag.shape, f32)
        for k in range(tap_count):
            values = jnp.where(lag == k, spread[m, :, pl.ds(k * 128, 128)], values)
        return values.astype(bf16)

    def rims_of(ch):
        rim = halo_in[ch]
        return jnp.concatenate(
            [jnp.where(fold_lane == q, rim, jnp.zeros_like(rim)) for q in range(folds)], axis=0
        )

    def filtered(filt, window):
        return lax.dot_general(
            filt, window, (((1,), (1,)), ((), ())), preferred_element_type=f32
        ).astype(bf16)

    def steered(ch, delayed):
        wr = w_buf[ch, pl.ds(0, antennas), :]
        wi = w_buf[ch, pl.ds(antennas, antennas), :]
        steer = jnp.concatenate(
            [jnp.concatenate([wr, wi], axis=1), jnp.concatenate([-wi, wr], axis=1)], axis=0
        )
        return jnp.dot(delayed, steer, preferred_element_type=f32)

    def beams_of(ch):
        @pl.when(lax.rem(ch, group) == 0)
        def _():
            halo_copy(ch).wait_recv()

        m = sets[0, ch]
        rim = toeplitz(m, rim_lag[...])
        rim = jnp.concatenate([rim, jnp.zeros((time_len - pad, time_len), bf16)], axis=0)
        filt = jnp.concatenate([toeplitz(m, own_lag[...]), rim], axis=1)
        window = jnp.concatenate([v_buf[ch], rims_of(ch)], axis=1)
        return steered(ch, filtered(filt, window))

    def pack(ch):
        span = pl.ds(ch, group)
        wide = jnp.concatenate(
            [
                v_buf[span, pl.ds(q * fold_rows, fold_rows), :].reshape(group * fold_rows, time_len)
                for q in range(folds)
            ],
            axis=1,
        )
        packed = jnp.dot(wide, picker, preferred_element_type=f32).astype(bf16)
        halo_out[span] = packed.reshape(group, fold_rows, time_len)
        halo_copy(ch).start()

    def late_rows_of(i):
        ch = ahead_channel(i)
        filt = toeplitz(sets[0, ch], own_lag[late_rows, :])
        total = steered(ch, filtered(filt, v_buf[ch]))
        acc_out[ch, late_rows, :] = total.astype(bf16)

    for copy in first_loads:
        copy.wait()

    if head:
        @pl.when(place == 0)
        def _():
            late_rows_of(0)

    present = len(sides) + jnp.where(me > 0, 1, 0) + jnp.where(me < n - 1, 1, 0)
    pl.semaphore_wait(barrier, present)

    def send_late(i, carry):
        late_rows_of(i)
        piece_copy(i, late_rows).start()
        return carry

    if head:
        @pl.when(place == 0)
        def _():
            piece_copy(0, late_rows).start()

            for copy in head_loads:
                copy.wait()

            lax.fori_loop(1, head, send_late, 0)

            pack(first)

    @pl.when(place > 0)
    def _():
        for copy in head_loads:
            copy.wait()

    for copy in load(0, channels - max(head, group), 2):
        copy.wait()

    def pack_first(g, carry):
        pack(ahead_channel(start + g * group))
        return carry

    lax.fori_loop(0, lead // group, pack_first, 0)

    if head:
        @pl.when(place == 0)
        def _():
            def send_early(i, carry):
                ch = ahead_channel(i)

                @pl.when(lax.rem(i, group) == 0)
                def _():
                    halo_copy(ch).wait_recv()

                m = sets[0, ch]
                filt = jnp.concatenate(
                    [toeplitz(m, own_lag[early_rows, :]), toeplitz(m, rim_lag[...])], axis=1
                )
                window = jnp.concatenate([v_buf[ch], rims_of(ch)], axis=1)
                total = steered(ch, filtered(filt, window))
                acc_out[ch, early_rows, :] = total.astype(bf16)
                piece_copy(i, early_rows).start()
                return carry

            lax.fori_loop(0, head, send_early, 0)

    def step(i, carry):
        j = i - offset

        @pl.when((i + lead < ahead_count) & (lax.rem(i, group) == 0))
        def _():
            pack(ahead_channel(i + lead))

        @pl.when((j + lead >= 0) & (j + lead < back_count) & (lax.rem(j + lead, group) == 0))
        def _():
            pack(back_channel(j + lead))

        @pl.when(i < ahead_count)
        def _():
            ch = ahead_channel(i)
            total = beams_of(ch)

            @pl.when(place > 0)
            def _():
                @pl.when(lax.rem(i, group) == 0)
                def _():
                    wait_group(ch)

                acc_out[ch] = (total + acc_in[ch].astype(f32)).astype(bf16)

            @pl.when(place == 0)
            def _():
                acc_out[ch] = total.astype(bf16)

            sum_copy(ch, ahead_dir, i >= single_from).start()

        @pl.when((j >= 0) & (j < back_count))
        def _():
            ch = back_channel(j)
            total = beams_of(ch)
            slot = arrival(ch, back_dir)

            @pl.when(lax.rem(j, group) == 0)
            def _():
                wait_group(slot)

            total = total + acc_in[slot].astype(f32)

            @pl.when(j < place * rows)
            def _():
                acc_out[ch] = total.astype(bf16)
                sum_copy(ch, back_dir).start()

            @pl.when(j >= place * rows)
            def _():
                own[lax.rem(j, rows)] = total

        return carry

    lax.fori_loop(start, ahead_count + LAG, step, 0)

    def drain():
        pltpu.make_async_remote_copy(
            src_ref=halo_out,
            dst_ref=halo_in,
            send_sem=hs_sem,
            recv_sem=hr_sem.at[0],
            device_id={"tm": later},
            device_id_type=MESH,
        ).wait_send()
        sent = pl.ds(0, (n - 1) * rows)
        pltpu.make_async_remote_copy(
            src_ref=acc_out.at[sent],
            dst_ref=acc_in.at[sent],
            send_sem=as_sem,
            recv_sem=ar_sem.at[0],
            device_id={"tm": later},
            device_id_type=MESH,
        ).wait_send()

    @pl.when(place > 0)
    def _():
        drain()

        def finish(k, carry):
            slot = arrival(me * rows + k, ahead_dir)
            @pl.when(k >= rows - tail)
            def _():
                wait_single(slot)

            @pl.when((k < rows - group) & (lax.rem(k, group) == 0))
            def _():
                wait_group(slot)

            if group > tail:
                @pl.when(k == rows - group)
                def _():
                    wait_group(slot, group - tail)

            out_buf[k] = (own[k] + acc_in[slot].astype(f32)).T.astype(bf16)
            return carry

        lax.fori_loop(0, rows, finish, 0)

    @pl.when(place == 0)
    def _():
        def finish(k, carry):
            out_buf[k] = own[k].T.astype(bf16)
            return carry

        lax.fori_loop(0, rows, finish, 0)
        drain()


def put_out(pieces, in_ref, out_ref, sem):
    size = in_ref.shape[0] // pieces
    for p in range(pieces):
        span = pl.ds(p * size, size)
        pltpu.make_async_copy(in_ref.at[span], out_ref.at[span], sem).start()
    pltpu.make_async_copy(in_ref, out_ref, sem).wait()


def body(voltages, delays, tap_sets, tap_table, weights):
    _, channels, parts, antennas, time_len = voltages.shape
    beams = weights.shape[-1]
    set_count, tap_count = tap_table.shape
    n = lax.axis_size("station")
    tm_count = lax.axis_size("tm")
    rows = channels // n
    pad = MAXD + tap_count
    rows_in = parts * antennas
    fold_rows = rows_in * pad // time_len
    group = max(rows // 2, 1)
    sizes = (channels, parts, antennas, beams, time_len, pad, group)
    bf16, f32 = jnp.bfloat16, jnp.float32
    dma = pltpu.SemaphoreType.DMA
    in_hbm = pl.BlockSpec(memory_space=pltpu.HBM)
    operands = (
        tap_sets,
        delays,
        tap_table,
        voltages.reshape(channels, rows_in, time_len),
        weights.reshape(channels, rows_in, beams),
    )
    result = pl.pallas_call(
        functools.partial(kernel, n, tm_count, sizes),
        out_shape=pltpu.VMEM((rows, 2 * beams, time_len), bf16),
        in_specs=[in_hbm] * 5,
        out_specs=pl.BlockSpec(memory_space=pltpu.VMEM),
        scratch_shapes=[
            pltpu.SMEM(tap_sets.shape, jnp.int32),
            pltpu.SMEM(delays.shape, jnp.int32),
            pltpu.VMEM((set_count, tap_count), bf16),
            pltpu.VMEM((set_count, 1, tap_count * 128), f32),
            pltpu.VMEM((time_len, time_len), jnp.int32),
            pltpu.VMEM((pad, time_len), jnp.int32),
            pltpu.VMEM((channels, rows_in, time_len), bf16),
            pltpu.VMEM((channels, rows_in, beams), bf16),
            pltpu.VMEM((channels, fold_rows, time_len), bf16),
            pltpu.VMEM((channels, fold_rows, time_len), bf16),
            pltpu.VMEM((channels, time_len, 2 * beams), bf16),
            pltpu.VMEM((channels + rows, time_len, 2 * beams), bf16),
            pltpu.VMEM((rows, time_len, 2 * beams), f32),
            dma((3,)),
            dma((6,)),
            dma(()),
            dma((channels // group,)),
            dma(()),
            dma(((channels + rows) // group + max(group // 2, 1),)),
        ],
        compiler_params=pltpu.CompilerParams(
            collective_id=0, has_side_effects=True, vmem_limit_bytes=40 * 1024 * 1024
        ),
    )(*(x if x.ndim == 1 else pltpu.with_memory_space_constraint(x, pltpu.HBM) for x in operands))
    result = pl.pallas_call(
        functools.partial(put_out, min(4, rows)),
        out_shape=pltpu.HBM((rows, 2 * beams, time_len), bf16),
        in_specs=[pl.BlockSpec(memory_space=pltpu.VMEM)],
        out_specs=in_hbm,
        scratch_shapes=[dma(())],
    )(pltpu.with_memory_space_constraint(result, pltpu.VMEM))
    return result.reshape(rows, 2, beams, time_len)


def solution(mesh):
    return jax.shard_map(
        body,
        mesh=mesh,
        in_specs=(
            P(("group", "station"), "chan", None, None, "tm"),
            P(("group", "station")),
            P(("group", "station"), "chan"),
            P(),
            P(("group", "station"), "chan", None, None, None),
        ),
        out_specs=P(("group", "chan", "station"), None, None, "tm"),
        check_vma=False,
    )
```
